512 devices in a mesh: section: 4 (over y_hi), dp: 32 (over x, z), space: 4 (over y_lo, core).
Axes of the slice: x: 4, y: 8 (y_hi: 4, y_lo: 2; y = y_hi * 2 + y_lo), z: 8, core: 2. Of those that a mesh axis runs over, the one named last changes fastest.
Arguments:
- enc_input: bfloat16 [4, 32, 32, 8, 8, 128], P('section', 'dp', None, 'space'), may hold values from -6 to 6
- dec_input: bfloat16 [4, 32, 32, 8, 8, 128], P('section', 'dp', None, None, 'space'), may hold values from -6 to 6
- dec_cotangent: bfloat16 [4, 32, 32, 8, 8, 128], P('section', 'dp', None, None, 'space'), may hold values from -6 to 6
- deep_cotangent: bfloat16 [4, 32, 32, 8, 8, 128], P('section', 'dp', None, 'space'), may hold values from -6 to 6
- enc_weight: bfloat16 [4, 27, 32, 32], P('section'), may hold values from -0.21875 to 0.21875
- dec_weight: bfloat16 [4, 27, 32, 64], P('section'), may hold values from -0.15625 to 0.15625
- enc_gain: float32 [4, 32], P('section'), may hold values from 0.25 to 1.75
- enc_bias: float32 [4, 32], P('section'), may hold values from -2 to 2
- dec_gain: float32 [4, 32], P('section'), may hold values from 0.25 to 1.75
- dec_bias: float32 [4, 32], P('section'), may hold values from -2 to 2
Outputs:
- enc_handoff: bfloat16 [4, 32, 32, 8, 8, 128], P('section', 'dp', None, 'space')
- dec_handoff: bfloat16 [4, 32, 32, 8, 8, 128], P('section', 'dp', None, None, 'space')
- enc_weight_grad: float32 [4, 27648], P('section', ('dp', 'space'))
- dec_weight_grad: float32 [4, 55296], P('section', ('dp', 'space'))
The draws below stay inside these ranges and needn't reach their ends.
All inputs are finite; a program needn't handle non-finite values.
Results may differ from the reference program's by a relative error of at most 0.0075.
Values may be sent and summed in bfloat16 or wider, within the bound.
A program may use at most 64 MiB of HBM per device.

```python
import math
import jax
import jax.numpy as jnp
from jax import lax

C = 32
W = 128
SECTIONS = 4
BATCH = 32
D = 8
H = 8
N_DP = 32


def levels(key, shape, cuts, least, top_value):
    loudness, own = 1.0, jax.random.fold_in(key, 6)
    for axis_at, shards_of in cuts:
        draws = jnp.exp(jax.random.uniform(jax.random.fold_in(own, axis_at), (shards_of,), jnp.float32, least / len(cuts), top_value / len(cuts)))
        loudness = loudness * jnp.repeat(draws, shape[axis_at] // shards_of).reshape([-1 if axis == axis_at else 1 for axis in range(len(shape))])
    return loudness


def centred(rng, dims, scale, limit, cuts=(), held_as=jnp.bfloat16):
    values = scale * jax.random.normal(rng, dims, jnp.float32)
    if cuts:
        values = values * levels(rng, dims, cuts, -0.22, 0.18)
    return jnp.clip(values, -limit, limit).astype(held_as)


def setup_inputs(seed: int = 0) -> dict:
    streams_of = jax.random.split(jax.random.key(seed), 11)
    enc_input = centred(streams_of[0], (SECTIONS, BATCH, C, D, H, W), 1.0, 6.0, ((0, 4), (1, 32), (3, 4)))
    dec_input = centred(streams_of[1], (SECTIONS, BATCH, C, D, H, W), 1.0, 6.0, ((0, 4), (1, 32), (4, 4)))
    dec_cotangent = centred(streams_of[2], (SECTIONS, BATCH, C, D, H, W), 1.0, 6.0, ((0, 4), (1, 32), (4, 4)))
    deep_cotangent = centred(streams_of[3], (SECTIONS, BATCH, C, D, H, W), 1.0, 6.0, ((0, 4), (1, 32), (3, 4)))
    enc_weight = centred(streams_of[4], (SECTIONS, 27, C, C), (27 * C) ** -0.5, 0.21875, ((0, 4),))
    dec_weight = centred(streams_of[5], (SECTIONS, 27, C, 2 * C), (54 * C) ** -0.5, 0.15625, ((0, 4),))
    enc_gain = jnp.clip(1.0 + 0.15 * jax.random.normal(streams_of[6], (SECTIONS, C), jnp.float32), 0.25, 1.75)
    enc_bias = centred(streams_of[7], (SECTIONS, C), 0.5, 2.0, ((0, 4),), jnp.float32)
    dec_gain = jnp.clip(1.0 + 0.15 * jax.random.normal(streams_of[8], (SECTIONS, C), jnp.float32), 0.25, 1.75)
    dec_bias = centred(streams_of[9], (SECTIONS, C), 0.5, 2.0, ((0, 4),), jnp.float32)
    return dict(enc_input=enc_input, dec_input=dec_input, dec_cotangent=dec_cotangent, deep_cotangent=deep_cotangent, enc_weight=enc_weight, dec_weight=dec_weight, enc_gain=enc_gain, enc_bias=enc_bias, dec_gain=dec_gain, dec_bias=dec_bias)


EPS = 1e-05

def convolve(padded, weights):
    depth_cells = padded.shape[1] - 2
    height_cells = padded.shape[2] - 2
    width_cells = padded.shape[3] - 2
    summed = jnp.zeros((weights.shape[1], depth_cells, height_cells, width_cells), jnp.float32)
    for tap_index in range(27):
        depth_tap = tap_index // 9
        height_tap = tap_index // 3 % 3
        width_tap = tap_index % 3
        window = padded[:, depth_tap:depth_tap + depth_cells, height_tap:height_tap + height_cells, width_tap:width_tap + width_cells]
        summed = summed + jnp.einsum('oi,idhw->odhw', weights[tap_index].astype(jnp.float32), window.astype(jnp.float32))
    return summed

def weight_terms(padded, cotangent):
    depth_cells = cotangent.shape[1]
    height_cells = cotangent.shape[2]
    width_cells = cotangent.shape[3]
    pieces = []
    for tap_index in range(27):
        depth_tap = tap_index // 9
        height_tap = tap_index // 3 % 3
        width_tap = tap_index % 3
        window = padded[:, depth_tap:depth_tap + depth_cells, height_tap:height_tap + height_cells, width_tap:width_tap + width_cells]
        pieces.append(jnp.einsum('odhw,idhw->oi', cotangent.astype(jnp.float32), window.astype(jnp.float32)))
    return jnp.stack(pieces)

def standardize(values):
    mean_value = lax.optimization_barrier(jnp.mean(values, axis=(1, 2, 3)))
    variance = lax.optimization_barrier(jnp.mean(values * values, axis=(1, 2, 3))) - mean_value * mean_value
    scaling = lax.rsqrt(variance + EPS)
    return ((values - mean_value[:, None, None, None]) * scaling[:, None, None, None], scaling)

def pad_all(volume):
    return jnp.pad(volume, ((0, 0), (1, 1), (1, 1), (1, 1)))

def one_crop(enc_in, dec_in, cot_in, deep_in, enc_w, dec_w, enc_g, enc_b, dec_g, dec_b):
    enc_padded = pad_all(enc_in)
    enc_pre = convolve(enc_padded, enc_w)
    enc_hat, enc_scale = standardize(enc_pre)
    enc_normed = enc_g[:, None, None, None] * enc_hat + enc_b[:, None, None, None]
    skip_act = jnp.maximum(enc_normed, 0.0).astype(jnp.bfloat16)
    joined = jnp.concatenate([dec_in, skip_act], axis=0)
    dec_padded = pad_all(joined)
    dec_pre = convolve(dec_padded, dec_w)
    dec_hat, unused_scale = standardize(dec_pre)
    dec_act = jnp.maximum(dec_g[:, None, None, None] * dec_hat + dec_b[:, None, None, None], 0.0).astype(jnp.bfloat16)
    dec_grad = weight_terms(dec_padded, cot_in)
    flipped = jnp.swapaxes(dec_w[::-1, :, C:], 1, 2)
    skip_grad = convolve(pad_all(cot_in), flipped).astype(jnp.bfloat16)
    upstream = skip_grad.astype(jnp.float32) + deep_in.astype(jnp.float32)
    gated = jnp.where(enc_normed > 0, upstream, 0.0) * enc_g[:, None, None, None]
    first_mean = lax.optimization_barrier(jnp.mean(gated, axis=(1, 2, 3)))[:, None, None, None]
    second_mean = lax.optimization_barrier(jnp.mean(gated * enc_hat, axis=(1, 2, 3)))[:, None, None, None]
    enc_pre_grad = ((gated - first_mean - enc_hat * second_mean) * enc_scale[:, None, None, None]).astype(jnp.bfloat16)
    enc_grad = weight_terms(enc_padded, enc_pre_grad)
    return (skip_act, dec_act, enc_grad, dec_grad)

def reference(enc_input, dec_input, dec_cotangent, deep_cotangent, enc_weight, dec_weight, enc_gain, enc_bias, dec_gain, dec_bias):
    grad_scale = 1.0 / math.sqrt(N_DP * D * H * W)

    def one_section(section_args):
        enc_in, dec_in, cot_in, deep_in, enc_w, dec_w, enc_g, enc_b, dec_g, dec_b = section_args

        def run_crop(crop_args):
            return one_crop(crop_args[0], crop_args[1], crop_args[2], crop_args[3], enc_w, dec_w, enc_g, enc_b, dec_g, dec_b)
        skips, decoded, enc_grads, dec_grads = lax.map(run_crop, (enc_in, dec_in, cot_in, deep_in))
        enc_total = lax.optimization_barrier(jnp.sum(enc_grads, axis=0)).reshape(-1) * grad_scale
        dec_total = lax.optimization_barrier(jnp.sum(dec_grads, axis=0)).reshape(-1) * grad_scale
        return (skips, decoded, enc_total, dec_total)
    skips, decoded, enc_total, dec_total = lax.map(one_section, (enc_input, dec_input, dec_cotangent, deep_cotangent, enc_weight, dec_weight, enc_gain, enc_bias, dec_gain, dec_bias))
    enc_handoff = jnp.concatenate([jnp.zeros_like(skips[:1]), skips[:-1]], axis=0)
    dec_handoff = jnp.concatenate([decoded[1:], jnp.zeros_like(decoded[:1])], axis=0)
    return (enc_handoff, dec_handoff, enc_total, dec_total)
```

```python
import math

import jax
import jax.numpy as jnp
from jax import lax
from jax.experimental import pallas as pl
from jax.experimental.pallas import tpu as pltpu
from jax.sharding import PartitionSpec as P

SPACE = "space"
DP = "dp"
DP_SPACE = ("dp", "space")


EPS = 1e-05


def padded_2(cells, sides, width):
    for axis, dim in sides:
        count = lax.axis_size(axis)
        ends = count - 1
        head = lax.slice_in_dim(cells, 0, width, axis=dim)
        tail = lax.slice_in_dim(cells, cells.shape[dim] - width, cells.shape[dim], axis=dim)
        cells = jnp.concatenate(
            [
                lax.ppermute(tail, axis, [(i, (i + 1) % count) for i in range(ends)]),
                cells,
                lax.ppermute(head, axis, [((i + 1) % count, i) for i in range(ends)]),
            ],
            axis=dim,
        )
    return cells


def copy_for_each(array, axis):
    count = lax.axis_size(axis)
    return lax.all_to_all(
        jnp.broadcast_to(array[None], (count, *array.shape)), axis, 0, 0, tiled=True
    )


def of_everyone(array, axis):
    return copy_for_each(array, axis).sum(axis=0)


def in_one(arrays, axis):
    ends = [0]
    for a in arrays:
        ends.append(ends[-1] + a.size)
    subtotal = of_everyone(jnp.concatenate([a.ravel() for a in arrays]), axis)
    return tuple((subtotal[b:e].reshape(a.shape) for a, b, e in zip(arrays, ends, ends[1:])))


def shifted_2(block, axis, distance):
    devices = range(lax.axis_size(axis))
    route = [(i - distance, i) for i in devices if i - distance in devices]
    return lax.ppermute(block, axis, route)


def reduce_kernel(n_dp, n_space, terms, total, arrived, near, partial, sent, got, near_sent, near_got):
    me = lax.axis_index(DP)
    slab = lax.axis_index(SPACE)
    barrier = pltpu.get_barrier_semaphore()

    def greet(i, carry):
        pl.semaphore_signal(barrier, inc=1, device_id={DP: lax.rem(me + i, n_dp)})
        return carry

    lax.fori_loop(1, n_dp, greet, 0)
    for i in range(1, n_space):
        pl.semaphore_signal(barrier, inc=1, device_id={SPACE: lax.rem(slab + i, n_space)})
    pl.semaphore_wait(barrier, n_dp + n_space - 2)

    def far_copy(i):
        peer = lax.rem(me + i, n_dp)
        return pltpu.make_async_remote_copy(
            src_ref=terms.at[peer],
            dst_ref=arrived.at[me],
            send_sem=sent.at[peer],
            recv_sem=got.at[me],
            device_id={DP: peer},
        )

    def far_arrival(i):
        peer = lax.rem(me - i + n_dp, n_dp)
        return peer, pltpu.make_async_remote_copy(
            src_ref=terms.at[peer],
            dst_ref=arrived.at[peer],
            send_sem=sent.at[peer],
            recv_sem=got.at[peer],
            device_id={DP: peer},
        )

    def start(i, carry):
        far_copy(i).start()
        return carry

    lax.fori_loop(1, n_dp, start, 0)

    def collect(i, acc):
        peer, copy = far_arrival(i)
        copy.wait_recv()
        return acc + arrived[peer]

    partial[...] = lax.fori_loop(1, n_dp, collect, terms[me])

    def near_copy(i):
        peer = lax.rem(slab + i, n_space)
        return pltpu.make_async_remote_copy(
            src_ref=partial,
            dst_ref=near.at[i - 1],
            send_sem=near_sent.at[i - 1],
            recv_sem=near_got.at[i - 1],
            device_id={SPACE: peer},
        )

    for i in range(1, n_space):
        near_copy(i).start()
    acc = partial[...]
    for i in range(1, n_space):
        near_copy(i).wait_recv()
        acc = acc + near[i - 1]
    total[...] = acc

    def drain(i, carry):
        far_copy(i).wait_send()
        return carry

    lax.fori_loop(1, n_dp, drain, 0)
    for i in range(1, n_space):
        near_copy(i).wait_send()


def reduced(enc_grad, dec_grad):
    n_dp, n_space = lax.axis_size(DP), lax.axis_size(SPACE)
    enc_terms = enc_grad.reshape(n_dp, -1)
    dec_terms = dec_grad.reshape(n_dp, -1)
    enc_width, dec_width = enc_terms.shape[1], dec_terms.shape[1]
    rows = -(-(enc_width + dec_width) // 1024) * 8
    terms = jnp.concatenate([enc_terms, dec_terms], axis=1)
    terms = jnp.pad(terms, ((0, 0), (0, rows * 128 - terms.shape[1]))).reshape(n_dp, rows, 128)
    vmem = pl.BlockSpec(memory_space=pltpu.VMEM)
    total = pl.pallas_call(
        lambda *refs: reduce_kernel(n_dp, n_space, *refs),
        out_shape=jax.ShapeDtypeStruct((rows, 128), jnp.float32),
        in_specs=[vmem],
        out_specs=vmem,
        scratch_shapes=[
            pltpu.VMEM((n_dp, rows, 128), jnp.float32),
            pltpu.VMEM((n_space - 1, rows, 128), jnp.float32),
            pltpu.VMEM((rows, 128), jnp.float32),
            pltpu.SemaphoreType.DMA((n_dp,)),
            pltpu.SemaphoreType.DMA((n_dp,)),
            pltpu.SemaphoreType.DMA((n_space - 1,)),
            pltpu.SemaphoreType.DMA((n_space - 1,)),
        ],
        compiler_params=pltpu.CompilerParams(collective_id=0, has_side_effects=True),
    )(terms).reshape(-1)
    slab = lax.axis_index(SPACE)
    enc_part = lax.dynamic_slice(total, (slab * (enc_width // n_space),), (enc_width // n_space,))
    dec_part = lax.dynamic_slice(
        total, (enc_width + slab * (dec_width // n_space),), (dec_width // n_space,)
    )
    return enc_part, dec_part


def convolve(padded, weights):
    depth_cells = padded.shape[1] - 2
    height_cells = padded.shape[2] - 2
    width_cells = padded.shape[3] - 2
    summed = jnp.zeros((weights.shape[1], depth_cells, height_cells, width_cells), jnp.float32)
    for depth_tap in range(3):
        for height_tap in range(3):
            shifted = jnp.stack(
                [
                    padded[
                        :,
                        depth_tap : depth_tap + depth_cells,
                        height_tap : height_tap + height_cells,
                        width_tap : width_tap + width_cells,
                    ]
                    for width_tap in range(3)
                ]
            )
            first = depth_tap * 9 + height_tap * 3
            tap_weights = weights[first : first + 3]
            summed = summed + jnp.einsum(
                "koi,kidhw->odhw", tap_weights, shifted, preferred_element_type=jnp.float32
            )
    return summed


def weight_terms(padded, cotangent):
    depth_cells = cotangent.shape[1]
    height_cells = cotangent.shape[2]
    width_cells = cotangent.shape[3]
    pieces = []
    for depth_tap in range(3):
        for height_tap in range(3):
            shifted = jnp.stack(
                [
                    padded[
                        :,
                        depth_tap : depth_tap + depth_cells,
                        height_tap : height_tap + height_cells,
                        width_tap : width_tap + width_cells,
                    ]
                    for width_tap in range(3)
                ]
            )
            pieces.append(
                jnp.einsum(
                    "odhw,kidhw->koi", cotangent, shifted, preferred_element_type=jnp.float32
                )
            )
    return jnp.concatenate(pieces, axis=0)


def channel_view(values):
    return values[:, None, None, None]


def body(
    enc_input,
    dec_input,
    dec_cotangent,
    deep_cotangent,
    enc_weight,
    dec_weight,
    enc_gain,
    enc_bias,
    dec_gain,
    dec_bias,
):
    volume = enc_input[0, 0]
    channels = volume.shape[0]
    slabs = lax.axis_size(SPACE)
    voxels = volume.shape[1] * slabs * volume.shape[2] * volume.shape[3]
    grad_scale = 1.0 / math.sqrt(lax.axis_size(DP) * voxels)
    enc_rimmed = padded_2(volume, ((SPACE, 1),), 1)
    enc_padded = jnp.pad(enc_rimmed, ((0, 0), (0, 0), (1, 1), (1, 1)))
    enc_pre = convolve(enc_padded, enc_weight[0])
    enc_sums, enc_squares = in_one(
        (jnp.sum(enc_pre, axis=(1, 2, 3)), jnp.sum(enc_pre * enc_pre, axis=(1, 2, 3))), SPACE
    )
    enc_mean = enc_sums / voxels
    enc_scale = lax.rsqrt(enc_squares / voxels - enc_mean * enc_mean + EPS)
    enc_hat = (enc_pre - channel_view(enc_mean)) * channel_view(enc_scale)
    enc_normed = channel_view(enc_gain[0]) * enc_hat + channel_view(enc_bias[0])
    skip_act = jnp.maximum(enc_normed, 0.0).astype(jnp.bfloat16)
    enc_handoff = shifted_2(skip_act[None, None], "section", 1)
    skip_high = lax.all_to_all(skip_act, SPACE, split_axis=2, concat_axis=1, tiled=True)
    joined = jnp.concatenate([dec_input[0, 0], skip_high], axis=0)
    dec_rimmed = padded_2(joined, ((SPACE, 2),), 1)
    dec_padded = jnp.pad(dec_rimmed, ((0, 0), (1, 1), (0, 0), (1, 1)))
    dec_pre = convolve(dec_padded, dec_weight[0])
    dec_sums, dec_squares = in_one(
        (jnp.sum(dec_pre, axis=(1, 2, 3)), jnp.sum(dec_pre * dec_pre, axis=(1, 2, 3))), SPACE
    )
    dec_mean = dec_sums / voxels
    dec_scale = lax.rsqrt(dec_squares / voxels - dec_mean * dec_mean + EPS)
    dec_hat = (dec_pre - channel_view(dec_mean)) * channel_view(dec_scale)
    dec_act = jnp.maximum(
        channel_view(dec_gain[0]) * dec_hat + channel_view(dec_bias[0]), 0.0
    ).astype(jnp.bfloat16)
    dec_handoff = shifted_2(dec_act[None, None], "section", -1)
    cotangent = dec_cotangent[0, 0]
    dec_grad = weight_terms(dec_padded, cotangent).reshape(-1) * grad_scale
    flipped = jnp.swapaxes(dec_weight[0][::-1, :, channels:], 1, 2)
    cot_rimmed = padded_2(cotangent, ((SPACE, 2),), 1)
    cot_padded = jnp.pad(cot_rimmed, ((0, 0), (1, 1), (0, 0), (1, 1)))
    grad_high = convolve(cot_padded, flipped).astype(jnp.bfloat16)
    skip_grad = lax.all_to_all(grad_high, SPACE, split_axis=1, concat_axis=2, tiled=True)
    upstream = skip_grad.astype(jnp.float32) + deep_cotangent[0, 0].astype(jnp.float32)
    gated = jnp.where(enc_normed > 0, upstream, 0.0) * channel_view(enc_gain[0])
    first_sum, second_sum = in_one(
        (jnp.sum(gated, axis=(1, 2, 3)), jnp.sum(gated * enc_hat, axis=(1, 2, 3))), SPACE
    )
    enc_pre_grad = (
        (gated - channel_view(first_sum / voxels) - enc_hat * channel_view(second_sum / voxels))
        * channel_view(enc_scale)
    ).astype(jnp.bfloat16)
    enc_grad = weight_terms(enc_padded, enc_pre_grad).reshape(-1) * grad_scale
    enc_part, dec_part = reduced(enc_grad, dec_grad)
    return (enc_handoff, dec_handoff, enc_part[None], dec_part[None])


def solution(mesh):
    placed = (
        P("section", DP, None, SPACE, None, None),
        P("section", DP, None, None, SPACE, None),
        P("section", DP, None, None, SPACE, None),
        P("section", DP, None, SPACE, None, None),
        P("section", None, None, None),
        P("section", None, None, None),
        P("section", None),
        P("section", None),
        P("section", None),
        P("section", None),
    )
    return jax.shard_map(
        body,
        mesh=mesh,
        in_specs=placed,
        out_specs=(
            P("section", DP, None, SPACE, None, None),
            P("section", DP, None, None, SPACE, None),
            P("section", DP_SPACE),
            P("section", DP_SPACE),
        ),
        check_vma=False,
    )
```

```python
import math

import jax
import jax.numpy as jnp
from jax import lax
from jax.experimental import pallas as pl
from jax.experimental.pallas import tpu as pltpu
from jax.sharding import PartitionSpec as P

SPACE = "space"
DP = "dp"
SECTION = "section"

EPS = 1e-05

C = 32
LANES = 128
FULL = 8
SPLIT = 2
ROWS = FULL * SPLIT
RUN = FULL * LANES
PADDED = (FULL + 2) * LANES
PAIR = SPLIT * LANES
TAPS = 9
WIDE = 3 * C
UNIT = TAPS * WIDE
ORDER = 11
SEND = jnp.bfloat16


def dot(a, b):
    return jnp.dot(a, b, preferred_element_type=jnp.float32)


def dot_t(a, b):
    return lax.dot_general(a, b, (((1,), (1,)), ((), ())), preferred_element_type=jnp.float32)


def lanes_of(shape):
    return lax.broadcasted_iota(jnp.int32, shape, len(shape) - 1)


def to_right(row):
    return jnp.where(lanes_of(row.shape) == 0, 0.0, pltpu.roll(row, 1, 1))


def to_left(row):
    return jnp.where(lanes_of(row.shape) == LANES - 1, 0.0, pltpu.roll(row, LANES - 1, 1))


def gather_taps(row):
    return jnp.concatenate([to_left(row), row, to_right(row)], axis=0).astype(jnp.bfloat16)


def merge_taps(wide):
    return to_right(wide[0:C]) + wide[C : 2 * C] + to_left(wide[2 * C : 3 * C])


def pack_stats(first, second):
    lanes = lanes_of((8, LANES))
    packed = jnp.zeros((8, LANES), jnp.float32)
    for k in range(4):
        for n, whole in enumerate((first, second)):
            part = whole[8 * k : 8 * k + 8]
            for shift in (64, 32, 16):
                part = part + pltpu.roll(part, shift, 1)
            low = 32 * k + 16 * n
            packed = jnp.where((lanes >= low) & (lanes < low + 16), part, packed)
    return packed


def unpack_stats(packed):
    lanes = lanes_of((8, LANES))
    both = []
    for n in range(2):
        pieces = []
        for k in range(4):
            low = 32 * k + 16 * n
            mine = jnp.where((lanes >= low) & (lanes < low + 16), packed, 0.0)
            pieces.append(jnp.sum(mine, axis=1, keepdims=True))
        both.append(jnp.concatenate(pieces, axis=0))
    return both


def kernel(
    n_section, n_dp, n_space, voxels, grad_scale,
    enc_in, dec_in, cot_in, deep_in, enc_w, dec_w, enc_gain, enc_bias, dec_gain, dec_bias,
    enc_out, dec_out, total,
    stage, back, x, xd, xs, cot, cot_halo, c3, e3, skip_send, sg, gr, deep, pre, dec_pre,
    prm, tr_w, stat_send, stat_got, grads, terms, arrived, near_send, near_got,
    enc_flat, dec_flat,
    halo_s, halo_r, stat_s, stat_r, skip_s, skip_r, sg_s, sg_r, own_sem,
    hand_s, hand_r, far_s, far_r, near_s, near_r,
):
    me = lax.axis_index(DP)
    slab = lax.axis_index(SPACE)
    level = lax.axis_index(SECTION)
    last = n_space - 1
    barrier = pltpu.get_barrier_semaphore()

    def greet(i, carry):
        pl.semaphore_signal(barrier, inc=1, device_id={DP: lax.rem(me + i, n_dp)})
        return carry

    for i in range(1, n_space):
        pl.semaphore_signal(barrier, inc=1, device_id={SPACE: lax.rem(slab + i, n_space)})
    lax.fori_loop(1, n_dp, greet, 0)

    @pl.when(level > 0)
    def _():
        pl.semaphore_signal(barrier, inc=1, device_id={SECTION: level - 1})

    @pl.when(level < n_section - 1)
    def _():
        pl.semaphore_signal(barrier, inc=1, device_id={SECTION: level + 1})

    stage[0] = enc_in[...].astype(jnp.float32)
    stage[1] = cot_in[...].astype(jnp.float32)
    stage[2] = dec_in[...].astype(jnp.float32)
    stage[3] = deep_in[...].astype(jnp.float32)

    def row_of(k, r):
        return stage[k, pl.ds(r, C, stride=ROWS), :]

    for ref in (x, xd, xs):
        ref[:, :, 0:LANES] = jnp.zeros((4, C, LANES), ref.dtype)
        ref[:, :, PADDED - LANES : PADDED] = jnp.zeros((4, C, LANES), ref.dtype)
    c3[:, :, 0:LANES] = jnp.zeros((4, WIDE, LANES), c3.dtype)
    c3[:, :, PADDED - LANES : PADDED] = jnp.zeros((4, WIDE, LANES), c3.dtype)
    for u in range(SPLIT):
        for v in range(FULL):
            at = slice((1 + v) * LANES, (2 + v) * LANES)
            x[1 + u, :, at] = row_of(0, u * FULL + v).astype(jnp.bfloat16)
            cot[u, :, v * LANES : (v + 1) * LANES] = row_of(1, v * SPLIT + u).astype(jnp.bfloat16)
            xd[1 + u, :, at] = row_of(2, v * SPLIT + u).astype(jnp.bfloat16)

    @pl.when(slab == 0)
    def _():
        x[0] = jnp.zeros((C, PADDED), x.dtype)
        xd[0] = jnp.zeros((C, PADDED), xd.dtype)
        cot_halo[0] = jnp.zeros((C, RUN), cot_halo.dtype)

    @pl.when(slab == last)
    def _():
        x[3] = jnp.zeros((C, PADDED), x.dtype)
        xd[3] = jnp.zeros((C, PADDED), xd.dtype)
        cot_halo[1] = jnp.zeros((C, RUN), cot_halo.dtype)

    inner = slice(LANES, LANES + RUN)

    def halo(k, up):
        src_u, dst_u, peer = (2, 0, slab + 1) if up else (1, 3, slab - 1)
        if k == 1:
            src, dst = cot.at[src_u - 1], cot_halo.at[0 if up else 1]
        else:
            ref = x if k == 0 else xd
            src, dst = ref.at[src_u, :, inner], ref.at[dst_u, :, inner]
        n = 2 * k + (0 if up else 1)
        return pltpu.make_async_remote_copy(
            src_ref=src, dst_ref=dst, send_sem=halo_s.at[n], recv_sem=halo_r.at[n],
            device_id={SPACE: peer},
        )

    pl.semaphore_wait(
        barrier, n_dp + n_space - 2 + lax.min(level, 1) + lax.min(n_section - 1 - level, 1)
    )

    @pl.when(slab < last)
    def _():
        for k in range(3):
            halo(k, True).start()

    @pl.when(slab > 0)
    def _():
        for k in range(3):
            halo(k, False).start()

    def halo_arrived(k):
        @pl.when(slab > 0)
        def _():
            halo(k, True).wait_recv()

        @pl.when(slab < last)
        def _():
            halo(k, False).wait_recv()

    zeros_row = jnp.zeros((LANES, LANES), jnp.float32)
    prm[...] = zeros_row
    prm[0:1, 0:C] = enc_gain[...]
    prm[1:2, 0:C] = enc_bias[...]
    prm[2:3, 0:C] = dec_gain[...]
    prm[3:4, 0:C] = dec_bias[...]
    columns = prm[...].T
    e_gain, e_bias = columns[0:C, 0:1], columns[0:C, 1:2]
    d_gain, d_bias = columns[0:C, 2:3], columns[0:C, 3:4]
    pick = (
        lax.broadcasted_iota(jnp.int32, (C, 2 * C), 1)
        == lax.broadcasted_iota(jnp.int32, (C, 2 * C), 0) + C
    ).astype(jnp.bfloat16)
    for t in range(TAPS):
        tr_w[t] = dot_t(pick, dec_w[t]).astype(jnp.bfloat16)
    for u in range(SPLIT):
        for v in range(FULL):
            c3[1 + u, :, (1 + v) * LANES : (2 + v) * LANES] = gather_taps(row_of(1, v * SPLIT + u))
            deep[v, :, u * LANES : (u + 1) * LANES] = row_of(3, u * FULL + v)

    zero = jnp.zeros((C, LANES), jnp.float32)
    chunk = 2

    halo_arrived(0)
    first, second = zero, zero
    for u in range(SPLIT):
        for q in range(0, FULL, chunk):
            acc = jnp.zeros((WIDE, chunk * LANES), jnp.float32)
            for a in range(3):
                for b in range(3):
                    at = (q + b) * LANES
                    acc = acc + dot(enc_w[3 * a + b], x[u + a, :, at : at + chunk * LANES])
            for r in range(chunk):
                row = merge_taps(acc[:, r * LANES : (r + 1) * LANES])
                pre[q + r, :, u * LANES : (u + 1) * LANES] = row
                first = first + row
                second = second + row * row

    def stat_copy(n, i):
        k = n * (n_space - 1) + i - 1
        return pltpu.make_async_remote_copy(
            src_ref=stat_send.at[n], dst_ref=stat_got.at[k],
            send_sem=stat_s.at[k], recv_sem=stat_r.at[k],
            device_id={SPACE: lax.rem(slab + i, n_space)},
        )

    def send_stats(n, first, second):
        stat_send[n] = pack_stats(first, second)
        for i in range(1, n_space):
            stat_copy(n, i).start()

    def all_stats(n):
        packed = stat_send[n]
        for i in range(1, n_space):
            stat_copy(n, i).wait_recv()
            packed = packed + stat_got[n * (n_space - 1) + i - 1]
        one, two = unpack_stats(packed)
        return one * (1.0 / voxels), two * (1.0 / voxels)

    send_stats(0, first, second)

    halo_arrived(1)
    for side, u in ((0, 0), (1, 3)):
        for v in range(FULL):
            row = cot_halo[side, :, v * LANES : (v + 1) * LANES].astype(jnp.float32)
            c3[u, :, (1 + v) * LANES : (2 + v) * LANES] = gather_taps(row)
    for u in range(SPLIT):
        for q in range(0, FULL, chunk):
            acc = jnp.zeros((C, chunk * LANES), jnp.float32)
            for a in range(3):
                for b in range(3):
                    at = (q + 2 - a) * LANES
                    acc = acc + dot(tr_w[3 * a + b], c3[u + 2 - b, :, at : at + chunk * LANES])
            sg[u, :, q * LANES : (q + chunk) * LANES] = acc.astype(jnp.bfloat16)

    def sg_copy(i):
        peer = lax.rem(slab + i, n_space)
        return pltpu.make_async_remote_copy(
            src_ref=sg.at[:, :, pl.ds(pl.multiple_of(peer * PAIR, LANES), PAIR)],
            dst_ref=gr.at[pl.ds(slab * SPLIT, SPLIT)],
            send_sem=sg_s.at[i - 1], recv_sem=sg_r.at[i - 1], device_id={SPACE: peer},
        )

    def sg_arrival(i):
        peer = lax.rem(slab - i + n_space, n_space)
        return pltpu.make_async_remote_copy(
            src_ref=sg.at[:, :, pl.ds(pl.multiple_of(peer * PAIR, LANES), PAIR)],
            dst_ref=gr.at[pl.ds(peer * SPLIT, SPLIT)],
            send_sem=sg_s.at[i - 1], recv_sem=sg_r.at[i - 1], device_id={SPACE: peer},
        )

    sg_own = pltpu.make_async_copy(
        sg.at[:, :, pl.ds(pl.multiple_of(slab * PAIR, LANES), PAIR)],
        gr.at[pl.ds(slab * SPLIT, SPLIT)],
        own_sem.at[0],
    )
    for i in range(1, n_space):
        sg_copy(i).start()
    sg_own.start()

    e_mean, e_square = all_stats(0)
    e_scale = lax.rsqrt(e_square - e_mean * e_mean + EPS)

    def enc_hat_of(v, u):
        return (pre[v, :, u * LANES : (u + 1) * LANES] - e_mean) * e_scale

    skip_send[0] = jnp.zeros((C, PAIR), jnp.bfloat16)
    skip_send[FULL + 1] = jnp.zeros((C, PAIR), jnp.bfloat16)
    for v in range(FULL):
        for u in range(SPLIT):
            act = jnp.maximum(e_gain * enc_hat_of(v, u) + e_bias, 0.0).astype(jnp.bfloat16)
            skip_send[1 + v, :, u * LANES : (u + 1) * LANES] = act
            back[0, pl.ds(u * FULL + v, C, stride=ROWS), :] = act.astype(jnp.float32)

    def skip_refs(source, target):
        return (
            skip_send.at[pl.ds(target * SPLIT, SPLIT + 2)],
            xs.at[:, :, pl.ds(pl.multiple_of((1 + source * SPLIT) * LANES, LANES), PAIR)],
        )

    def skip_copy(i):
        peer = lax.rem(slab + i, n_space)
        src, dst = skip_refs(slab, peer)
        return pltpu.make_async_remote_copy(
            src_ref=src, dst_ref=dst, send_sem=skip_s.at[i - 1], recv_sem=skip_r.at[i - 1],
            device_id={SPACE: peer},
        )

    def skip_arrival(i):
        peer = lax.rem(slab - i + n_space, n_space)
        src, dst = skip_refs(peer, slab)
        return pltpu.make_async_remote_copy(
            src_ref=src, dst_ref=dst, send_sem=skip_s.at[i - 1], recv_sem=skip_r.at[i - 1],
            device_id={SPACE: peer},
        )

    skip_own = pltpu.make_async_copy(*skip_refs(slab, slab), own_sem.at[1])
    for i in range(1, n_space):
        skip_copy(i).start()
    skip_own.start()
    enc_flat[...] = back[0].astype(jnp.bfloat16)

    for i in range(1, n_space):
        sg_arrival(i).wait_recv()
    sg_own.wait()

    def gated_of(v, u, hat):
        at = slice(u * LANES, (u + 1) * LANES)
        upstream = gr[v, :, at].astype(jnp.float32) + deep[v, :, at]
        return jnp.where(e_gain * hat + e_bias > 0, upstream, 0.0) * e_gain

    first, second = zero, zero
    for v in range(FULL):
        for u in range(SPLIT):
            hat = enc_hat_of(v, u)
            gated = gated_of(v, u, hat)
            first = first + gated
            second = second + gated * hat
    send_stats(1, first, second)

    lanes8 = lanes_of((8, LANES))
    per_peer = UNIT // n_dp
    group = -(-per_peer // 4)

    def send_unit(n, left, right):
        for a in range(3):
            for b in range(3):
                acc = jnp.zeros((WIDE, C), jnp.float32)
                for u in range(SPLIT):
                    acc = acc + dot_t(left(u), right(u, a, b))
                t = 3 * a + b
                grads[n, t * WIDE : (t + 1) * WIDE, 0:C] = acc * grad_scale
        for p in range(n_dp):
            block = grads[n, p * per_peer : p * per_peer + 8, :]
            for g in range(1, 4):
                at = p * per_peer + g * group
                moved = pltpu.roll(grads[n, at : at + 8, :], 32 * g, 1)
                block = jnp.where(lanes8 < 32 * g, block, moved)
            terms[n, p] = block.astype(SEND)

        def start(i, carry):
            far_copy(n, i).start()
            return carry

        lax.fori_loop(1, n_dp, start, 0)

    def far_copy(n, i):
        peer = lax.rem(me + i * ORDER, n_dp)
        return pltpu.make_async_remote_copy(
            src_ref=terms.at[n, peer], dst_ref=arrived.at[n, me],
            send_sem=far_s.at[n, peer], recv_sem=far_r.at[n, me], device_id={DP: peer},
        )

    def far_arrival(n, i):
        peer = lax.rem(me - i * ORDER + n_dp * ORDER, n_dp)
        return peer, pltpu.make_async_remote_copy(
            src_ref=terms.at[n, peer], dst_ref=arrived.at[n, peer],
            send_sem=far_s.at[n, peer], recv_sem=far_r.at[n, peer], device_id={DP: peer},
        )

    halo_arrived(2)
    send_unit(
        1,
        lambda u: c3[1 + u, :, inner],
        lambda u, a, b: xd[u + b, :, a * LANES : a * LANES + RUN],
    )

    for i in range(1, n_space):
        skip_arrival(i).wait_recv()
    skip_own.wait()
    first, second = zero, zero
    for u in range(SPLIT):
        for q in range(0, FULL, chunk):
            acc = jnp.zeros((WIDE, chunk * LANES), jnp.float32)
            for a in range(3):
                for b in range(3):
                    at = slice((q + a) * LANES, (q + a + chunk) * LANES)
                    joined = jnp.concatenate([xd[u + b, :, at], xs[u + b, :, at]], axis=0)
                    acc = acc + dot(dec_w[3 * a + b], joined)
            for r in range(chunk):
                row = merge_taps(acc[:, r * LANES : (r + 1) * LANES])
                dec_pre[u, :, (q + r) * LANES : (q + r + 1) * LANES] = row
                first = first + row
                second = second + row * row
    send_stats(2, first, second)

    def hand(k):
        src, dst, step = (enc_flat, enc_out, 1) if k == 0 else (dec_flat, dec_out, -1)
        return pltpu.make_async_remote_copy(
            src_ref=src, dst_ref=dst, send_sem=hand_s.at[k], recv_sem=hand_r.at[k],
            device_id={SECTION: level + step},
        )

    @pl.when(level < n_section - 1)
    def _():
        hand(0).start()

    g_mean, gh_mean = all_stats(1)
    for u in range(SPLIT):
        for v in range(FULL):
            hat = enc_hat_of(v, u)
            row = (gated_of(v, u, hat) - g_mean - hat * gh_mean) * e_scale
            row = row.astype(jnp.bfloat16).astype(jnp.float32)
            e3[u, :, v * LANES : (v + 1) * LANES] = gather_taps(row)
    send_unit(
        0,
        lambda u: e3[u],
        lambda u, a, b: x[u + a, :, b * LANES : b * LANES + RUN],
    )
    send_unit(
        2,
        lambda u: c3[1 + u, :, inner],
        lambda u, a, b: xs[u + b, :, a * LANES : a * LANES + RUN],
    )

    d_mean, d_square = all_stats(2)
    d_scale = lax.rsqrt(d_square - d_mean * d_mean + EPS)
    for u in range(SPLIT):
        for v in range(FULL):
            hat = (dec_pre[u, :, v * LANES : (v + 1) * LANES] - d_mean) * d_scale
            back[1, pl.ds(v * SPLIT + u, C, stride=ROWS), :] = jnp.maximum(
                d_gain * hat + d_bias, 0.0
            )
    dec_flat[...] = back[1].astype(jnp.bfloat16)

    @pl.when(level > 0)
    def _():
        hand(1).start()

    @pl.when(level == 0)
    def _():
        enc_out[...] = jnp.zeros(enc_out.shape, enc_out.dtype)

    @pl.when(level == n_section - 1)
    def _():
        dec_out[...] = jnp.zeros(dec_out.shape, dec_out.dtype)

    for n in range(3):
        def collect(i, acc):
            peer, copy = far_arrival(n, i)
            copy.wait_recv()
            return acc + arrived[n, peer].astype(jnp.float32)

        near_send[n] = lax.fori_loop(1, n_dp, collect, terms[n, me].astype(jnp.float32))

    def near_copy(i):
        return pltpu.make_async_remote_copy(
            src_ref=near_send, dst_ref=near_got.at[i - 1],
            send_sem=near_s.at[i - 1], recv_sem=near_r.at[i - 1],
            device_id={SPACE: lax.rem(slab + i, n_space)},
        )

    for i in range(1, n_space):
        near_copy(i).start()
    acc = near_send[...]
    for i in range(1, n_space):
        near_copy(i).wait_recv()
        acc = acc + near_got[i - 1]
    total[...] = acc

    @pl.when(level > 0)
    def _():
        hand(0).wait_recv()
        hand(1).wait_send()

    @pl.when(level < n_section - 1)
    def _():
        hand(1).wait_recv()
        hand(0).wait_send()

    @pl.when(slab < last)
    def _():
        for k in range(3):
            halo(k, True).wait_send()

    @pl.when(slab > 0)
    def _():
        for k in range(3):
            halo(k, False).wait_send()

    for i in range(1, n_space):
        for n in range(3):
            stat_copy(n, i).wait_send()
        sg_copy(i).wait_send()
        skip_copy(i).wait_send()
        near_copy(i).wait_send()
    for n in range(3):
        def drain(i, carry):
            far_copy(n, i).wait_send()
            return carry

        lax.fori_loop(1, n_dp, drain, 0)


def body(
    enc_input, dec_input, dec_cotangent, deep_cotangent,
    enc_weight, dec_weight, enc_gain, enc_bias, dec_gain, dec_bias,
):
    n_section, n_dp, n_space = (lax.axis_size(a) for a in (SECTION, DP, SPACE))
    voxels = enc_input.shape[3] * n_space * enc_input.shape[4] * enc_input.shape[5]
    grad_scale = 1.0 / math.sqrt(n_dp * voxels)
    flat = (C * ROWS, LANES)
    vmem = pl.BlockSpec(memory_space=pltpu.VMEM)
    bf16, f32 = jnp.bfloat16, jnp.float32
    dma = pltpu.SemaphoreType.DMA
    others = n_space - 1
    enc_out, dec_out, total = pl.pallas_call(
        lambda *refs: kernel(n_section, n_dp, n_space, voxels, grad_scale, *refs),
        out_shape=(
            jax.ShapeDtypeStruct(flat, bf16),
            jax.ShapeDtypeStruct(flat, bf16),
            jax.ShapeDtypeStruct((3, 8, LANES), f32),
        ),
        in_specs=[vmem] * 10,
        out_specs=(vmem, vmem, vmem),
        scratch_shapes=[
            pltpu.VMEM((4, *flat), f32),
            pltpu.VMEM((2, *flat), f32),
            pltpu.VMEM((4, C, PADDED), bf16),
            pltpu.VMEM((4, C, PADDED), bf16),
            pltpu.VMEM((4, C, PADDED), bf16),
            pltpu.VMEM((SPLIT, C, RUN), bf16),
            pltpu.VMEM((2, C, RUN), bf16),
            pltpu.VMEM((4, WIDE, PADDED), bf16),
            pltpu.VMEM((SPLIT, WIDE, RUN), bf16),
            pltpu.VMEM((FULL + 2, C, PAIR), bf16),
            pltpu.VMEM((SPLIT, C, RUN), bf16),
            pltpu.VMEM((FULL, C, PAIR), bf16),
            pltpu.VMEM((FULL, C, PAIR), f32),
            pltpu.VMEM((FULL, C, PAIR), f32),
            pltpu.VMEM((SPLIT, C, RUN), f32),
            pltpu.VMEM((LANES, LANES), f32),
            pltpu.VMEM((TAPS, C, WIDE), bf16),
            pltpu.VMEM((3, 8, LANES), f32),
            pltpu.VMEM((3 * others, 8, LANES), f32),
            pltpu.VMEM((3, UNIT + 8, LANES), f32),
            pltpu.VMEM((3, n_dp, 8, LANES), SEND),
            pltpu.VMEM((3, n_dp, 8, LANES), SEND),
            pltpu.VMEM((3, 8, LANES), f32),
            pltpu.VMEM((others, 3, 8, LANES), f32),
            pltpu.VMEM(flat, bf16),
            pltpu.VMEM(flat, bf16),
            dma((6,)), dma((6,)),
            dma((3 * others,)), dma((3 * others,)),
            dma((others,)), dma((others,)),
            dma((others,)), dma((others,)),
            dma((2,)),
            dma((2,)), dma((2,)),
            dma((3, n_dp)), dma((3, n_dp)),
            dma((others,)), dma((others,)),
        ],
        compiler_params=pltpu.CompilerParams(
            collective_id=0, has_side_effects=True, vmem_limit_bytes=48 * 1024 * 1024
        ),
    )(
        enc_input.reshape(flat), dec_input.reshape(flat), dec_cotangent.reshape(flat),
        deep_cotangent.reshape(flat), enc_weight.reshape(TAPS, WIDE, C),
        dec_weight.reshape(TAPS, WIDE, 2 * C), enc_gain, enc_bias, dec_gain, dec_bias,
    )
    per_peer = UNIT // n_dp
    group = -(-per_peer // 4)
    units = total[:, :group].reshape(3, group, 4, C).transpose(0, 2, 1, 3)
    units = units.reshape(3, 4 * group, C)[:, :per_peer]
    slab = lax.axis_index(SPACE)
    enc_sums = units[0].reshape(n_space, -1)
    dec_sums = jnp.concatenate([units[1], units[2]], axis=1).reshape(n_space, -1)
    return (
        enc_out.reshape(enc_input.shape),
        dec_out.reshape(dec_input.shape),
        lax.dynamic_index_in_dim(enc_sums, slab, 0),
        lax.dynamic_index_in_dim(dec_sums, slab, 0),
    )


def solution(mesh):
    by_depth = P(SECTION, DP, None, SPACE, None, None)
    by_height = P(SECTION, DP, None, None, SPACE, None)
    whole3, whole1 = P(SECTION, None, None, None), P(SECTION, None)
    return jax.shard_map(
        body,
        mesh=mesh,
        in_specs=(by_depth, by_height, by_height, by_depth, whole3, whole3, *[whole1] * 4),
        out_specs=(by_depth, by_height, P(SECTION, (DP, SPACE)), P(SECTION, (DP, SPACE))),
        check_vma=False,
    )
```

```python
import math

import jax
import jax.numpy as jnp
from jax import lax
from jax.experimental import pallas as pl
from jax.experimental.pallas import tpu as pltpu
from jax.sharding import PartitionSpec as P

SPACE = "space"
DP = "dp"
SECTION = "section"

EPS = 1e-05

C = 32
LANES = 128
FULL = 8
SPLIT = 2
ROWS = FULL * SPLIT
RUN = FULL * LANES
PADDED = (FULL + 2) * LANES
PAIR = SPLIT * LANES
TAPS = 9
WIDE = 3 * C
UNIT = TAPS * WIDE
ORDER = 11
SEND = jnp.bfloat16


def dot(a, b):
    return jnp.dot(a, b, preferred_element_type=jnp.float32)


def dot_t(a, b):
    return lax.dot_general(a, b, (((1,), (1,)), ((), ())), preferred_element_type=jnp.float32)


def lanes_of(shape):
    return lax.broadcasted_iota(jnp.int32, shape, len(shape) - 1)


def to_right(row):
    return jnp.where(lanes_of(row.shape) == 0, 0.0, pltpu.roll(row, 1, 1))


def to_left(row):
    return jnp.where(lanes_of(row.shape) == LANES - 1, 0.0, pltpu.roll(row, LANES - 1, 1))


def gather_taps(row):
    return jnp.concatenate([to_left(row), row, to_right(row)], axis=0).astype(jnp.bfloat16)


def merge_taps(wide):
    return to_right(wide[0:C]) + wide[C : 2 * C] + to_left(wide[2 * C : 3 * C])


def pack_stats(first, second):
    lanes = lanes_of((8, LANES))
    packed = jnp.zeros((8, LANES), jnp.float32)
    for k in range(4):
        for n, whole in enumerate((first, second)):
            part = whole[8 * k : 8 * k + 8]
            for shift in (64, 32, 16):
                part = part + pltpu.roll(part, shift, 1)
            low = 32 * k + 16 * n
            packed = jnp.where((lanes >= low) & (lanes < low + 16), part, packed)
    return packed


def pack_pair(first, second):
    lanes = lanes_of((8, LANES))
    packed = jnp.zeros((8, LANES), jnp.float32)
    for k in range(4):
        for n, whole in enumerate((first, second)):
            low = 32 * k + 16 * n
            mine = (lanes >= low) & (lanes < low + 16)
            packed = jnp.where(mine, whole[8 * k : 8 * k + 8], packed)
    return packed


def unpack(packed, width):
    lanes = lanes_of((8, LANES))
    both = []
    for n in range(2):
        pieces = []
        for k in range(4):
            low = 32 * k + 16 * n
            mine = jnp.where((lanes >= low) & (lanes < low + width), packed, 0.0)
            pieces.append(jnp.sum(mine, axis=1, keepdims=True))
        both.append(jnp.concatenate(pieces, axis=0))
    return both


def kernel(
    n_section, n_dp, n_space, voxels, grad_scale,
    enc_hbm, dec_hbm, cot_hbm, deep_hbm, enc_w_hbm, dec_w_hbm, g0, g1, g2, g3,
    enc_out, dec_out, total,
    loaded, enc_w, dec_w, params,
    stage, back, x, xd, xs, xc, cot_send, c3, c3e, e3, skip_send, sg, deep, pre, dec_pre,
    prm, tr_w, stat_send, stat_got, grads, terms, arrived, near_send, near_got,
    enc_flat, dec_raw, dec_got, coef_send, coef_got,
    load_s, halo_s, halo_r, stat_s, stat_r, skip_s, skip_r, cot_s, cot_r, own_sem,
    hand_s, hand_r, far_s, far_r, near_s, near_r,
):
    me = lax.axis_index(DP)
    slab = lax.axis_index(SPACE)
    level = lax.axis_index(SECTION)
    last = n_space - 1
    cells = ROWS * LANES

    loads = [
        pltpu.make_async_copy(src, dst, load_s.at[n])
        for n, (src, dst) in enumerate(
            (
                (enc_hbm, loaded.at[0]), (cot_hbm, loaded.at[1]), (enc_w_hbm, enc_w),
                (dec_hbm, loaded.at[2]), (deep_hbm, loaded.at[3]), (dec_w_hbm, dec_w),
                (g0, params.at[0]), (g1, params.at[1]), (g2, params.at[2]), (g3, params.at[3]),
            )
        )
    ]
    for load in loads:
        load.start()

    barrier = pltpu.get_barrier_semaphore()

    def greet(i, carry):
        pl.semaphore_signal(barrier, inc=1, device_id={DP: lax.rem(me + i, n_dp)})
        return carry

    for i in range(1, n_space):
        pl.semaphore_signal(barrier, inc=1, device_id={SPACE: lax.rem(slab + i, n_space)})
    lax.fori_loop(1, n_dp, greet, 0)

    @pl.when(level > 0)
    def _():
        pl.semaphore_signal(barrier, inc=1, device_id={SECTION: level - 1})

    @pl.when(level < n_section - 1)
    def _():
        pl.semaphore_signal(barrier, inc=1, device_id={SECTION: level + 1})

    def row_of(k, r):
        return stage[k, pl.ds(r, C, stride=ROWS), :]

    def lane(r, n=1):
        return slice(r * LANES, (r + n) * LANES)

    inner = lane(1, FULL)

    for ref in (x, xd, xs, xc):
        ref[:, :, lane(0)] = jnp.zeros((4, C, LANES), ref.dtype)
        ref[:, :, lane(FULL + 1)] = jnp.zeros((4, C, LANES), ref.dtype)
    c3e[:, :, lane(0)] = jnp.zeros((4, WIDE, LANES), c3e.dtype)
    c3e[:, :, lane(FULL + 1)] = jnp.zeros((4, WIDE, LANES), c3e.dtype)
    for ref in (skip_send, cot_send):
        ref[0] = jnp.zeros((C, PAIR), ref.dtype)
        ref[FULL + 1] = jnp.zeros((C, PAIR), ref.dtype)

    @pl.when(slab == 0)
    def _():
        x[0] = jnp.zeros((C, PADDED), x.dtype)
        xd[0] = jnp.zeros((C, PADDED), xd.dtype)

    @pl.when(slab == last)
    def _():
        x[3] = jnp.zeros((C, PADDED), x.dtype)
        xd[3] = jnp.zeros((C, PADDED), xd.dtype)

    loads[0].wait()
    stage[0] = loaded[0].astype(jnp.float32)
    for u in range(SPLIT):
        for v in range(FULL):
            x[1 + u, :, lane(1 + v)] = row_of(0, u * FULL + v).astype(jnp.bfloat16)
    loads[1].wait()
    stage[1] = loaded[1].astype(jnp.float32)
    for u in range(SPLIT):
        for v in range(FULL):
            cot_send[1 + v, :, lane(u)] = row_of(1, v * SPLIT + u).astype(jnp.bfloat16)
    loads[3].wait()
    stage[2] = loaded[2].astype(jnp.float32)
    for u in range(SPLIT):
        for v in range(FULL):
            xd[1 + u, :, lane(1 + v)] = row_of(2, v * SPLIT + u).astype(jnp.bfloat16)

    def halo(k, up):
        src_u, dst_u, peer = (2, 0, slab + 1) if up else (1, 3, slab - 1)
        ref = (x, xd)[k]
        n = 2 * k + (0 if up else 1)
        return pltpu.make_async_remote_copy(
            src_ref=ref.at[src_u, :, inner], dst_ref=ref.at[dst_u, :, inner],
            send_sem=halo_s.at[n], recv_sem=halo_r.at[n], device_id={SPACE: peer},
        )

    def halo_start(k):
        @pl.when(slab < last)
        def _():
            halo(k, True).start()

        @pl.when(slab > 0)
        def _():
            halo(k, False).start()

    def halo_arrived(k):
        @pl.when(slab > 0)
        def _():
            halo(k, True).wait_recv()

        @pl.when(slab < last)
        def _():
            halo(k, False).wait_recv()

    def regroup(sender, receiver, send_sem, recv_sem, own):
        def refs(source, target):
            at = pl.multiple_of((1 + source * SPLIT) * LANES, LANES)
            return (
                sender.at[pl.ds(target * SPLIT, SPLIT + 2)],
                receiver.at[:, :, pl.ds(at, PAIR)],
            )

        def copy(i):
            peer = lax.rem(slab + i, n_space)
            src, dst = refs(slab, peer)
            return pltpu.make_async_remote_copy(
                src_ref=src, dst_ref=dst, send_sem=send_sem.at[i - 1],
                recv_sem=recv_sem.at[i - 1], device_id={SPACE: peer},
            )

        def arrival(i):
            peer = lax.rem(slab - i + n_space, n_space)
            src, dst = refs(peer, slab)
            return pltpu.make_async_remote_copy(
                src_ref=src, dst_ref=dst, send_sem=send_sem.at[i - 1],
                recv_sem=recv_sem.at[i - 1], device_id={SPACE: peer},
            )

        return copy, arrival, pltpu.make_async_copy(*refs(slab, slab), own)

    cot_copy, cot_arrival, cot_own = regroup(cot_send, xc, cot_s, cot_r, own_sem.at[0])
    skip_copy, skip_arrival, skip_own = regroup(skip_send, xs, skip_s, skip_r, own_sem.at[1])

    pl.semaphore_wait(
        barrier, n_dp + n_space - 2 + lax.min(level, 1) + lax.min(n_section - 1 - level, 1)
    )
    halo_start(0)
    for i in range(1, n_space):
        cot_copy(i).start()
    cot_own.start()
    halo_start(1)

    for n in (6, 7, 8, 9):
        loads[n].wait()
    prm[...] = jnp.zeros((LANES, LANES), jnp.float32)
    for n in range(4):
        prm[n : n + 1, 0:C] = params[n]
    columns = prm[...].T
    e_gain, e_bias = columns[0:C, 0:1], columns[0:C, 1:2]
    d_gain, d_bias = columns[0:C, 2:3], columns[0:C, 3:4]
    pick = (
        lax.broadcasted_iota(jnp.int32, (C, 2 * C), 1)
        == lax.broadcasted_iota(jnp.int32, (C, 2 * C), 0) + C
    ).astype(jnp.bfloat16)
    loads[5].wait()
    for t in range(TAPS):
        tr_w[t] = dot_t(pick, dec_w[t]).astype(jnp.bfloat16)
    loads[4].wait()
    stage[3] = loaded[3].astype(jnp.float32)
    for u in range(SPLIT):
        for v in range(FULL):
            c3[u, :, lane(v)] = gather_taps(row_of(1, v * SPLIT + u))
            deep[v, :, lane(u)] = row_of(3, u * FULL + v)
    loads[2].wait()

    zero = jnp.zeros((C, LANES), jnp.float32)
    chunk = 2

    halo_arrived(0)
    first, second = zero, zero
    for u in range(SPLIT):
        for q in range(0, FULL, chunk):
            acc = jnp.zeros((WIDE, chunk * LANES), jnp.float32)
            for a in range(3):
                for b in range(3):
                    acc = acc + dot(enc_w[3 * a + b], x[u + a, :, lane(q + b, chunk)])
            for r in range(chunk):
                row = merge_taps(acc[:, lane(r)])
                pre[q + r, :, lane(u)] = row
                first = first + row
                second = second + row * row

    def stat_copy(n, i):
        k = n * (n_space - 1) + i - 1
        return pltpu.make_async_remote_copy(
            src_ref=stat_send.at[n], dst_ref=stat_got.at[n, slab],
            send_sem=stat_s.at[k], recv_sem=stat_r.at[k],
            device_id={SPACE: lax.rem(slab + i, n_space)},
        )

    def stat_arrival(n, i):
        k = n * (n_space - 1) + i - 1
        peer = lax.rem(slab - i + n_space, n_space)
        return pltpu.make_async_remote_copy(
            src_ref=stat_send.at[n], dst_ref=stat_got.at[n, peer],
            send_sem=stat_s.at[k], recv_sem=stat_r.at[k], device_id={SPACE: peer},
        )

    def send_stats(n, first, second):
        packed = pack_stats(first, second)
        stat_send[n] = packed
        for i in range(1, n_space):
            stat_copy(n, i).start()
        stat_got[n, slab] = packed
        return packed

    def all_stats(n):
        for i in range(1, n_space):
            stat_arrival(n, i).wait_recv()
        packed = stat_got[n, 0]
        for j in range(1, n_space):
            packed = packed + stat_got[n, j]
        one, two = unpack(packed, 16)
        return one * (1.0 / voxels), two * (1.0 / voxels)

    packed = send_stats(0, first, second)
    own_mean = unpack(packed, 16)[0] * (1.0 / cells)
    for v in range(FULL):
        for u in range(SPLIT):
            skip_send[1 + v, :, lane(u)] = (pre[v, :, lane(u)] - own_mean).astype(jnp.bfloat16)
    for i in range(1, n_space):
        skip_copy(i).start()
    skip_own.start()

    for i in range(1, n_space):
        cot_arrival(i).wait_recv()
    cot_own.wait()
    for u in range(4):
        for v in range(FULL):
            c3e[u, :, lane(1 + v)] = gather_taps(xc[u, :, lane(1 + v)].astype(jnp.float32))
    for u in range(SPLIT):
        for q in range(0, FULL, chunk):
            acc = jnp.zeros((C, chunk * LANES), jnp.float32)
            for a in range(3):
                for b in range(3):
                    acc = acc + dot(tr_w[3 * a + b], c3e[u + 2 - a, :, lane(q + 2 - b, chunk)])
            for r in range(chunk):
                sg[q + r, :, lane(u)] = acc[:, lane(r)].astype(jnp.bfloat16)

    e_mean, e_square = all_stats(0)
    e_scale = lax.rsqrt(e_square - e_mean * e_mean + EPS)

    def enc_hat_of(v, u):
        return (pre[v, :, lane(u)] - e_mean) * e_scale

    def gated_of(v, u, hat):
        upstream = sg[v, :, lane(u)].astype(jnp.float32) + deep[v, :, lane(u)]
        return jnp.where(e_gain * hat + e_bias > 0, upstream, 0.0) * e_gain

    first, second = zero, zero
    for v in range(FULL):
        for u in range(SPLIT):
            hat = enc_hat_of(v, u)
            gated = gated_of(v, u, hat)
            first = first + gated
            second = second + gated * hat
    send_stats(1, first, second)
    for v in range(FULL):
        for u in range(SPLIT):
            back[0, pl.ds(u * FULL + v, C, stride=ROWS), :] = jnp.maximum(
                e_gain * enc_hat_of(v, u) + e_bias, 0.0
            )
    enc_flat[...] = back[0].astype(jnp.bfloat16)

    lanes8 = lanes_of((8, LANES))
    per_peer = UNIT // n_dp

    def send_unit(n, left, right):
        for a in range(3):
            for b in range(3):
                acc = jnp.zeros((WIDE, C), jnp.float32)
                for u in range(SPLIT):
                    acc = acc + dot_t(left(u), right(u, a, b))
                t = 3 * a + b
                grads[n, t * WIDE : (t + 1) * WIDE, 0:C] = acc * grad_scale
        for p in range(n_dp):
            block = grads[n, pl.ds(p * per_peer, 8, stride=4), :]
            for g in range(1, 4):
                rows = grads[n, pl.ds(p * per_peer + g, 8, stride=4), :]
                block = jnp.where(lanes8 < 32 * g, block, pltpu.roll(rows, 32 * g, 1))
            terms[n, p] = block.astype(SEND)

        def start(i, carry):
            far_copy(n, i).start()
            return carry

        lax.fori_loop(1, n_dp, start, 0)

    def far_copy(n, i):
        peer = lax.rem(me + i * ORDER, n_dp)
        return pltpu.make_async_remote_copy(
            src_ref=terms.at[n, peer], dst_ref=arrived.at[n, me],
            send_sem=far_s.at[n, peer], recv_sem=far_r.at[n, me], device_id={DP: peer},
        )

    def far_arrival(n, i):
        peer = lax.rem(me - i * ORDER + n_dp * ORDER, n_dp)
        return peer, pltpu.make_async_remote_copy(
            src_ref=terms.at[n, peer], dst_ref=arrived.at[n, peer],
            send_sem=far_s.at[n, peer], recv_sem=far_r.at[n, peer], device_id={DP: peer},
        )

    halo_arrived(1)
    send_unit(1, lambda u: c3[u], lambda u, a, b: xd[u + b, :, lane(a, FULL)])

    gain = e_gain * e_scale
    for i in range(1, n_space):
        skip_arrival(i).wait_recv()
    skip_own.wait()
    for j in range(n_space):
        shift = gain * (unpack(stat_got[0, j], 16)[0] * (1.0 / cells) - e_mean) + e_bias
        for w in range(SPLIT):
            at = lane(1 + SPLIT * j + w)
            for u in range(4):
                act = jnp.maximum(gain * xs[u, :, at].astype(jnp.float32) + shift, 0.0)
                if u == 0:
                    act = jnp.where(slab > 0, act, 0.0)
                if u == 3:
                    act = jnp.where(slab < last, act, 0.0)
                xs[u, :, at] = act.astype(jnp.bfloat16)

    first, second = zero, zero
    for u in range(SPLIT):
        for q in range(0, FULL, chunk):
            acc = jnp.zeros((WIDE, chunk * LANES), jnp.float32)
            for a in range(3):
                for b in range(3):
                    at = lane(q + a, chunk)
                    joined = jnp.concatenate([xd[u + b, :, at], xs[u + b, :, at]], axis=0)
                    acc = acc + dot(dec_w[3 * a + b], joined)
            for r in range(chunk):
                row = merge_taps(acc[:, lane(r)])
                dec_pre[u, :, lane(q + r)] = row
                first = first + row
                second = second + row * row
    packed = send_stats(2, first, second)
    own_mean = unpack(packed, 16)[0] * (1.0 / cells)
    for u in range(SPLIT):
        for v in range(FULL):
            dec_raw[u, :, lane(v)] = (dec_pre[u, :, lane(v)] - own_mean).astype(jnp.bfloat16)

    def hand(k):
        src, dst, step = ((enc_flat, enc_out, 1), (dec_raw, dec_got, -1), (coef_send, coef_got, -1))[k]
        return pltpu.make_async_remote_copy(
            src_ref=src, dst_ref=dst, send_sem=hand_s.at[k], recv_sem=hand_r.at[k],
            device_id={SECTION: level + step},
        )

    @pl.when(level > 0)
    def _():
        hand(1).start()

    @pl.when(level < n_section - 1)
    def _():
        hand(0).start()

    g_mean, gh_mean = all_stats(1)
    for u in range(SPLIT):
        for v in range(FULL):
            hat = enc_hat_of(v, u)
            row = (gated_of(v, u, hat) - g_mean - hat * gh_mean) * e_scale
            row = row.astype(jnp.bfloat16).astype(jnp.float32)
            e3[u, :, lane(v)] = gather_taps(row)
    send_unit(0, lambda u: e3[u], lambda u, a, b: x[u + a, :, lane(b, FULL)])
    send_unit(2, lambda u: c3[u], lambda u, a, b: xs[u + b, :, lane(a, FULL)])

    d_mean, d_square = all_stats(2)
    d_gain = d_gain * lax.rsqrt(d_square - d_mean * d_mean + EPS)
    coef_send[...] = pack_pair(d_gain, d_gain * (own_mean - d_mean) + d_bias)

    @pl.when(level > 0)
    def _():
        hand(2).start()

    @pl.when(level == 0)
    def _():
        enc_out[...] = jnp.zeros(enc_out.shape, enc_out.dtype)

    for n in (1, 0, 2):
        def collect(i, acc):
            peer, copy = far_arrival(n, i)
            copy.wait_recv()
            return acc + arrived[n, peer].astype(jnp.float32)

        near_send[n] = lax.fori_loop(1, n_dp, collect, terms[n, me].astype(jnp.float32))

    def near_copy(i):
        return pltpu.make_async_remote_copy(
            src_ref=near_send, dst_ref=near_got.at[i - 1],
            send_sem=near_s.at[i - 1], recv_sem=near_r.at[i - 1],
            device_id={SPACE: lax.rem(slab + i, n_space)},
        )

    for i in range(1, n_space):
        near_copy(i).start()

    @pl.when(level < n_section - 1)
    def _():
        hand(1).wait_recv()
        hand(2).wait_recv()
        scale, shift = unpack(coef_got[...], 1)
        for u in range(SPLIT):
            for v in range(FULL):
                back[1, pl.ds(v * SPLIT + u, C, stride=ROWS), :] = jnp.maximum(
                    scale * dec_got[u, :, lane(v)].astype(jnp.float32) + shift, 0.0
                )
        dec_out[...] = back[1].astype(jnp.bfloat16)

    @pl.when(level == n_section - 1)
    def _():
        dec_out[...] = jnp.zeros(dec_out.shape, dec_out.dtype)

    acc = near_send[...]
    for i in range(1, n_space):
        near_copy(i).wait_recv()
        acc = acc + near_got[i - 1]
    total[...] = acc

    @pl.when(level > 0)
    def _():
        hand(0).wait_recv()
        hand(1).wait_send()
        hand(2).wait_send()

    @pl.when(level < n_section - 1)
    def _():
        hand(0).wait_send()

    @pl.when(slab < last)
    def _():
        for k in range(2):
            halo(k, True).wait_send()

    @pl.when(slab > 0)
    def _():
        for k in range(2):
            halo(k, False).wait_send()

    for i in range(1, n_space):
        for n in range(3):
            stat_copy(n, i).wait_send()
        cot_copy(i).wait_send()
        skip_copy(i).wait_send()
        near_copy(i).wait_send()
    for n in range(3):
        def drain(i, carry):
            far_copy(n, i).wait_send()
            return carry

        lax.fori_loop(1, n_dp, drain, 0)


def finish(n_space, enc_in, dec_in, sums, enc_hbm, dec_hbm, enc_grad, dec_grad, sems):
    slab = lax.axis_index(SPACE)
    copies = [
        pltpu.make_async_copy(enc_in, enc_hbm, sems.at[0]),
        pltpu.make_async_copy(dec_in, dec_hbm, sems.at[1]),
    ]
    for copy in copies:
        copy.start()

    def part(rows, out):
        flat = jnp.concatenate(rows, axis=1)
        width = out.shape[1]
        mine = flat[:, 0:width]
        for j in range(1, n_space):
            mine = jnp.where(slab == j, flat[:, j * width : (j + 1) * width], mine)
        out[...] = mine

    part([sums[0, r : r + 1, :] for r in range(7)], enc_grad)
    own, skip = sums[1], sums[2]
    group = lanes_of((8, LANES)) // C
    even = jnp.where(
        group == 0, own,
        jnp.where(
            group == 1, pltpu.roll(skip, 32, 1),
            jnp.where(group == 2, pltpu.roll(own, 32, 1), pltpu.roll(skip, 64, 1)),
        ),
    )
    odd = jnp.where(
        group == 0, pltpu.roll(own, 64, 1),
        jnp.where(
            group == 1, pltpu.roll(skip, 96, 1),
            jnp.where(group == 2, pltpu.roll(own, 96, 1), skip),
        ),
    )
    rows = []
    for r in range(7):
        rows += [even[r : r + 1, :], odd[r : r + 1, :]]
    part(rows, dec_grad)
    for copy in copies:
        copy.wait()


def body(
    enc_input, dec_input, dec_cotangent, deep_cotangent,
    enc_weight, dec_weight, enc_gain, enc_bias, dec_gain, dec_bias,
):
    n_section, n_dp, n_space = (lax.axis_size(a) for a in (SECTION, DP, SPACE))
    voxels = enc_input.shape[3] * n_space * enc_input.shape[4] * enc_input.shape[5]
    grad_scale = 1.0 / math.sqrt(n_dp * voxels)
    flat = (C * ROWS, LANES)
    vmem = pl.BlockSpec(memory_space=pltpu.VMEM)
    hbm = pl.BlockSpec(memory_space=pltpu.HBM)
    bf16, f32 = jnp.bfloat16, jnp.float32
    dma = pltpu.SemaphoreType.DMA
    others = n_space - 1
    enc_out, dec_out, total = pl.pallas_call(
        lambda *refs: kernel(n_section, n_dp, n_space, voxels, grad_scale, *refs),
        out_shape=(
            pltpu.VMEM(flat, bf16),
            pltpu.VMEM(flat, bf16),
            pltpu.VMEM((3, 8, LANES), f32),
        ),
        in_specs=[hbm] * 10,
        out_specs=(vmem, vmem, vmem),
        scratch_shapes=[
            pltpu.VMEM((4, *flat), bf16),
            pltpu.VMEM((TAPS, WIDE, C), bf16),
            pltpu.VMEM((TAPS, WIDE, 2 * C), bf16),
            pltpu.VMEM((4, 1, C), f32),
            pltpu.VMEM((4, *flat), f32),
            pltpu.VMEM((2, *flat), f32),
            pltpu.VMEM((4, C, PADDED), bf16),
            pltpu.VMEM((4, C, PADDED), bf16),
            pltpu.VMEM((4, C, PADDED), bf16),
            pltpu.VMEM((4, C, PADDED), bf16),
            pltpu.VMEM((FULL + 2, C, PAIR), bf16),
            pltpu.VMEM((SPLIT, WIDE, RUN), bf16),
            pltpu.VMEM((4, WIDE, PADDED), bf16),
            pltpu.VMEM((SPLIT, WIDE, RUN), bf16),
            pltpu.VMEM((FULL + 2, C, PAIR), bf16),
            pltpu.VMEM((FULL, C, PAIR), bf16),
            pltpu.VMEM((FULL, C, PAIR), f32),
            pltpu.VMEM((FULL, C, PAIR), f32),
            pltpu.VMEM((SPLIT, C, RUN), f32),
            pltpu.VMEM((LANES, LANES), f32),
            pltpu.VMEM((TAPS, C, WIDE), bf16),
            pltpu.VMEM((3, 8, LANES), f32),
            pltpu.VMEM((3, n_space, 8, LANES), f32),
            pltpu.VMEM((3, UNIT + 8, LANES), f32),
            pltpu.VMEM((3, n_dp, 8, LANES), SEND),
            pltpu.VMEM((3, n_dp, 8, LANES), SEND),
            pltpu.VMEM((3, 8, LANES), f32),
            pltpu.VMEM((others, 3, 8, LANES), f32),
            pltpu.VMEM(flat, bf16),
            pltpu.VMEM((SPLIT, C, RUN), bf16),
            pltpu.VMEM((SPLIT, C, RUN), bf16),
            pltpu.VMEM((8, LANES), f32),
            pltpu.VMEM((8, LANES), f32),
            dma((10,)),
            dma((4,)), dma((4,)),
            dma((3 * others,)), dma((3 * others,)),
            dma((others,)), dma((others,)),
            dma((others,)), dma((others,)),
            dma((2,)),
            dma((3,)), dma((3,)),
            dma((3, n_dp)), dma((3, n_dp)),
            dma((others,)), dma((others,)),
        ],
        compiler_params=pltpu.CompilerParams(
            collective_id=0, has_side_effects=True, vmem_limit_bytes=48 * 1024 * 1024
        ),
    )(
        *(
            pltpu.with_memory_space_constraint(array, pltpu.HBM)
            for array in (
                enc_input.reshape(flat), dec_input.reshape(flat), dec_cotangent.reshape(flat),
                deep_cotangent.reshape(flat), enc_weight.reshape(TAPS, WIDE, C),
                dec_weight.reshape(TAPS, WIDE, 2 * C), enc_gain, enc_bias, dec_gain, dec_bias,
            )
        )
    )
    enc_width, dec_width = UNIT * C // (n_dp * n_space), 2 * UNIT * C // (n_dp * n_space)
    enc_out, dec_out, enc_grad, dec_grad = pl.pallas_call(
        lambda *refs: finish(n_space, *refs),
        out_shape=(
            jax.ShapeDtypeStruct(flat, bf16),
            jax.ShapeDtypeStruct(flat, bf16),
            jax.ShapeDtypeStruct((1, enc_width), f32),
            jax.ShapeDtypeStruct((1, dec_width), f32),
        ),
        in_specs=[vmem] * 3,
        out_specs=(hbm, hbm, vmem, vmem),
        scratch_shapes=[dma((2,))],
        compiler_params=pltpu.CompilerParams(vmem_limit_bytes=4 * 1024 * 1024),
    )(enc_out, dec_out, total)
    return (
        enc_out.reshape(enc_input.shape), dec_out.reshape(dec_input.shape), enc_grad, dec_grad
    )


def solution(mesh):
    by_depth = P(SECTION, DP, None, SPACE, None, None)
    by_height = P(SECTION, DP, None, None, SPACE, None)
    whole3, whole1 = P(SECTION, None, None, None), P(SECTION, None)
    return jax.shard_map(
        body,
        mesh=mesh,
        in_specs=(by_depth, by_height, by_height, by_depth, whole3, whole3, *[whole1] * 4),
        out_specs=(by_depth, by_height, P(SECTION, (DP, SPACE)), P(SECTION, (DP, SPACE))),
        check_vma=False,
    )
```

```python
import math

import jax
import jax.numpy as jnp
from jax import lax
from jax.experimental import pallas as pl
from jax.experimental.pallas import tpu as pltpu
from jax.sharding import PartitionSpec as P

SPACE = "space"
DP = "dp"
SECTION = "section"

EPS = 1e-05

C = 32
LANES = 128
FULL = 8
SPLIT = 2
ROWS = FULL * SPLIT
RUN = FULL * LANES
PADDED = (FULL + 2) * LANES
PAIR = SPLIT * LANES
TAPS = 9
WIDE = 3 * C
UNIT = TAPS * WIDE
RING = 8
ORDER = 11
SEND = jnp.bfloat16


def dot(a, b):
    return jnp.dot(a, b, preferred_element_type=jnp.float32)


def dot_t(a, b):
    return lax.dot_general(a, b, (((1,), (1,)), ((), ())), preferred_element_type=jnp.float32)


def lanes_of(shape):
    return lax.broadcasted_iota(jnp.int32, shape, len(shape) - 1)


def to_right(row):
    return jnp.where(lanes_of(row.shape) == 0, 0.0, pltpu.roll(row, 1, 1))


def to_left(row):
    return jnp.where(lanes_of(row.shape) == LANES - 1, 0.0, pltpu.roll(row, LANES - 1, 1))


def gather_taps(row):
    return jnp.concatenate([to_left(row), row, to_right(row)], axis=0).astype(jnp.bfloat16)


def merge_taps(wide):
    return to_right(wide[0:C]) + wide[C : 2 * C] + to_left(wide[2 * C : 3 * C])


def pack_stats(first, second):
    lanes = lanes_of((8, LANES))
    packed = jnp.zeros((8, LANES), jnp.float32)
    for k in range(4):
        for n, whole in enumerate((first, second)):
            part = whole[8 * k : 8 * k + 8]
            for shift in (64, 32, 16):
                part = part + pltpu.roll(part, shift, 1)
            low = 32 * k + 16 * n
            packed = jnp.where((lanes >= low) & (lanes < low + 16), part, packed)
    return packed


def pack_pair(first, second):
    lanes = lanes_of((8, LANES))
    packed = jnp.zeros((8, LANES), jnp.float32)
    for k in range(4):
        for n, whole in enumerate((first, second)):
            low = 32 * k + 16 * n
            mine = (lanes >= low) & (lanes < low + 16)
            packed = jnp.where(mine, whole[8 * k : 8 * k + 8], packed)
    return packed


def unpack(packed, width):
    lanes = lanes_of((8, LANES))
    both = []
    for n in range(2):
        pieces = []
        for k in range(4):
            low = 32 * k + 16 * n
            mine = jnp.where((lanes >= low) & (lanes < low + width), packed, 0.0)
            pieces.append(jnp.sum(mine, axis=1, keepdims=True))
        both.append(jnp.concatenate(pieces, axis=0))
    return both


def kernel(
    n_section, n_dp, n_space, voxels, grad_scale,
    enc_hbm, dec_hbm, cot_hbm, deep_hbm, enc_w_hbm, dec_w_hbm, g0, g1, g2, g3,
    enc_out, dec_out, total,
    loaded, enc_w, dec_w, params,
    stage, back, x, xd, xs, xc, cot_send, c3, c3e, e3, skip_send, sg, deep, pre, dec_pre,
    prm, tr_w, stat_send, stat_got, grads, terms, arrived, near_send, near_got,
    enc_flat, dec_raw, dec_got, coef_send, coef_got,
    load_s, halo_s, halo_r, stat_s, stat_r, skip_s, skip_r, cot_s, cot_r, own_sem,
    hand_s, hand_r, far_s, far_r, near_s, near_r, known,
):
    me = lax.axis_index(DP)
    slab = lax.axis_index(SPACE)
    level = lax.axis_index(SECTION)
    last = n_space - 1
    cells = ROWS * LANES

    loads = [
        pltpu.make_async_copy(src, dst, load_s.at[n])
        for n, (src, dst) in enumerate(
            (
                (enc_hbm, loaded.at[0]), (cot_hbm, loaded.at[1]), (enc_w_hbm, enc_w),
                (dec_hbm, loaded.at[2]), (deep_hbm, loaded.at[3]), (dec_w_hbm, dec_w),
                (g0, params.at[0]), (g1, params.at[1]), (g2, params.at[2]), (g3, params.at[3]),
            )
        )
    ]
    for load in loads:
        load.start()

    barrier = pltpu.get_barrier_semaphore()

    ring = min(RING, n_dp)
    far, near = lax.div(me, ring), lax.rem(me, ring)

    def along(step):
        return far * ring + lax.rem(near + step + ring, ring)

    def across(step):
        return lax.rem(far + step + n_dp // ring, n_dp // ring) * ring + near

    def tell(sem, peers):
        for peer in peers:
            pl.semaphore_signal(sem, inc=1, device_id={DP: peer})

    def heard(n):
        pl.semaphore_wait(known.at[n], 2)

    for i in range(1, n_space):
        pl.semaphore_signal(barrier, inc=1, device_id={SPACE: lax.rem(slab + i, n_space)})
    tell(barrier, (along(1), along(-1), across(1), across(-1)))

    @pl.when(level > 0)
    def _():
        pl.semaphore_signal(barrier, inc=1, device_id={SECTION: level - 1})

    @pl.when(level < n_section - 1)
    def _():
        pl.semaphore_signal(barrier, inc=1, device_id={SECTION: level + 1})

    def row_of(k, r):
        return stage[k, pl.ds(r, C, stride=ROWS), :]

    def lane(r, n=1):
        return slice(r * LANES, (r + n) * LANES)

    inner = lane(1, FULL)

    for ref in (x, xd, xs, xc):
        ref[:, :, lane(0)] = jnp.zeros((4, C, LANES), ref.dtype)
        ref[:, :, lane(FULL + 1)] = jnp.zeros((4, C, LANES), ref.dtype)
    c3e[:, :, lane(0)] = jnp.zeros((4, WIDE, LANES), c3e.dtype)
    c3e[:, :, lane(FULL + 1)] = jnp.zeros((4, WIDE, LANES), c3e.dtype)
    for ref in (skip_send, cot_send):
        ref[0] = jnp.zeros((C, PAIR), ref.dtype)
        ref[FULL + 1] = jnp.zeros((C, PAIR), ref.dtype)

    @pl.when(slab == 0)
    def _():
        x[0] = jnp.zeros((C, PADDED), x.dtype)
        xd[0] = jnp.zeros((C, PADDED), xd.dtype)

    @pl.when(slab == last)
    def _():
        x[3] = jnp.zeros((C, PADDED), x.dtype)
        xd[3] = jnp.zeros((C, PADDED), xd.dtype)

    loads[0].wait()
    stage[0] = loaded[0].astype(jnp.float32)
    for u in range(SPLIT):
        for v in range(FULL):
            x[1 + u, :, lane(1 + v)] = row_of(0, u * FULL + v).astype(jnp.bfloat16)
    loads[1].wait()
    stage[1] = loaded[1].astype(jnp.float32)
    for u in range(SPLIT):
        for v in range(FULL):
            cot_send[1 + v, :, lane(u)] = row_of(1, v * SPLIT + u).astype(jnp.bfloat16)
    loads[3].wait()
    stage[2] = loaded[2].astype(jnp.float32)
    for u in range(SPLIT):
        for v in range(FULL):
            xd[1 + u, :, lane(1 + v)] = row_of(2, v * SPLIT + u).astype(jnp.bfloat16)

    def halo(k, up):
        src_u, dst_u, peer = (2, 0, slab + 1) if up else (1, 3, slab - 1)
        ref = (x, xd)[k]
        n = 2 * k + (0 if up else 1)
        return pltpu.make_async_remote_copy(
            src_ref=ref.at[src_u, :, inner], dst_ref=ref.at[dst_u, :, inner],
            send_sem=halo_s.at[n], recv_sem=halo_r.at[n], device_id={SPACE: peer},
        )

    def halo_start(k):
        @pl.when(slab < last)
        def _():
            halo(k, True).start()

        @pl.when(slab > 0)
        def _():
            halo(k, False).start()

    def halo_arrived(k):
        @pl.when(slab > 0)
        def _():
            halo(k, True).wait_recv()

        @pl.when(slab < last)
        def _():
            halo(k, False).wait_recv()

    def regroup(sender, receiver, send_sem, recv_sem, own):
        def refs(source, target):
            at = pl.multiple_of((1 + source * SPLIT) * LANES, LANES)
            return (
                sender.at[pl.ds(target * SPLIT, SPLIT + 2)],
                receiver.at[:, :, pl.ds(at, PAIR)],
            )

        def copy(i):
            peer = lax.rem(slab + i, n_space)
            src, dst = refs(slab, peer)
            return pltpu.make_async_remote_copy(
                src_ref=src, dst_ref=dst, send_sem=send_sem.at[i - 1],
                recv_sem=recv_sem.at[i - 1], device_id={SPACE: peer},
            )

        def arrival(i):
            peer = lax.rem(slab - i + n_space, n_space)
            src, dst = refs(peer, slab)
            return pltpu.make_async_remote_copy(
                src_ref=src, dst_ref=dst, send_sem=send_sem.at[i - 1],
                recv_sem=recv_sem.at[i - 1], device_id={SPACE: peer},
            )

        return copy, arrival, pltpu.make_async_copy(*refs(slab, slab), own)

    cot_copy, cot_arrival, cot_own = regroup(cot_send, xc, cot_s, cot_r, own_sem.at[0])
    skip_copy, skip_arrival, skip_own = regroup(skip_send, xs, skip_s, skip_r, own_sem.at[1])

    pl.semaphore_wait(
        barrier, 4 + n_space - 1 + lax.min(level, 1) + lax.min(n_section - 1 - level, 1)
    )
    halo_start(0)
    for i in range(1, n_space):
        cot_copy(i).start()
    cot_own.start()
    halo_start(1)
    tell(known.at[0], (along(1), along(-1)))

    for n in (6, 7, 8, 9):
        loads[n].wait()
    prm[...] = jnp.zeros((LANES, LANES), jnp.float32)
    for n in range(4):
        prm[n : n + 1, 0:C] = params[n]
    columns = prm[...].T
    e_gain, e_bias = columns[0:C, 0:1], columns[0:C, 1:2]
    d_gain, d_bias = columns[0:C, 2:3], columns[0:C, 3:4]
    pick = (
        lax.broadcasted_iota(jnp.int32, (C, 2 * C), 1)
        == lax.broadcasted_iota(jnp.int32, (C, 2 * C), 0) + C
    ).astype(jnp.bfloat16)
    loads[5].wait()
    for t in range(TAPS):
        tr_w[t] = dot_t(pick, dec_w[t]).astype(jnp.bfloat16)
    loads[4].wait()
    stage[3] = loaded[3].astype(jnp.float32)
    for u in range(SPLIT):
        for v in range(FULL):
            c3[u, :, lane(v)] = gather_taps(row_of(1, v * SPLIT + u))
            deep[v, :, lane(u)] = row_of(3, u * FULL + v)
    loads[2].wait()
    heard(0)
    tell(known.at[1], (along(2), along(-2)))

    zero = jnp.zeros((C, LANES), jnp.float32)
    chunk = 2

    halo_arrived(0)
    first, second = zero, zero
    for u in range(SPLIT):
        for q in range(0, FULL, chunk):
            acc = jnp.zeros((WIDE, chunk * LANES), jnp.float32)
            for a in range(3):
                for b in range(3):
                    acc = acc + dot(enc_w[3 * a + b], x[u + a, :, lane(q + b, chunk)])
            for r in range(chunk):
                row = merge_taps(acc[:, lane(r)])
                pre[q + r, :, lane(u)] = row
                first = first + row
                second = second + row * row

    def stat_copy(n, i):
        k = n * (n_space - 1) + i - 1
        return pltpu.make_async_remote_copy(
            src_ref=stat_send.at[n], dst_ref=stat_got.at[n, slab],
            send_sem=stat_s.at[k], recv_sem=stat_r.at[k],
            device_id={SPACE: lax.rem(slab + i, n_space)},
        )

    def stat_arrival(n, i):
        k = n * (n_space - 1) + i - 1
        peer = lax.rem(slab - i + n_space, n_space)
        return pltpu.make_async_remote_copy(
            src_ref=stat_send.at[n], dst_ref=stat_got.at[n, peer],
            send_sem=stat_s.at[k], recv_sem=stat_r.at[k], device_id={SPACE: peer},
        )

    def send_stats(n, first, second):
        packed = pack_stats(first, second)
        stat_send[n] = packed
        for i in range(1, n_space):
            stat_copy(n, i).start()
        stat_got[n, slab] = packed
        return packed

    def all_stats(n):
        for i in range(1, n_space):
            stat_arrival(n, i).wait_recv()
        packed = stat_got[n, 0]
        for j in range(1, n_space):
            packed = packed + stat_got[n, j]
        one, two = unpack(packed, 16)
        return one * (1.0 / voxels), two * (1.0 / voxels)

    packed = send_stats(0, first, second)
    own_mean = unpack(packed, 16)[0] * (1.0 / cells)
    for v in range(FULL):
        for u in range(SPLIT):
            skip_send[1 + v, :, lane(u)] = (pre[v, :, lane(u)] - own_mean).astype(jnp.bfloat16)
    for i in range(1, n_space):
        skip_copy(i).start()
    skip_own.start()
    heard(1)
    tell(known.at[2], (across(1), across(-1)))

    for i in range(1, n_space):
        cot_arrival(i).wait_recv()
    cot_own.wait()
    for u in range(4):
        for v in range(FULL):
            c3e[u, :, lane(1 + v)] = gather_taps(xc[u, :, lane(1 + v)].astype(jnp.float32))
    for u in range(SPLIT):
        for q in range(0, FULL, chunk):
            acc = jnp.zeros((C, chunk * LANES), jnp.float32)
            for a in range(3):
                for b in range(3):
                    acc = acc + dot(tr_w[3 * a + b], c3e[u + 2 - a, :, lane(q + 2 - b, chunk)])
            for r in range(chunk):
                sg[q + r, :, lane(u)] = acc[:, lane(r)].astype(jnp.bfloat16)

    heard(2)
    tell(known.at[3], (across(1), across(-1)))

    e_mean, e_square = all_stats(0)
    e_scale = lax.rsqrt(e_square - e_mean * e_mean + EPS)

    def enc_hat_of(v, u):
        return (pre[v, :, lane(u)] - e_mean) * e_scale

    def gated_of(v, u, hat):
        upstream = sg[v, :, lane(u)].astype(jnp.float32) + deep[v, :, lane(u)]
        return jnp.where(e_gain * hat + e_bias > 0, upstream, 0.0) * e_gain

    first, second = zero, zero
    for v in range(FULL):
        for u in range(SPLIT):
            hat = enc_hat_of(v, u)
            gated = gated_of(v, u, hat)
            first = first + gated
            second = second + gated * hat
    send_stats(1, first, second)
    for v in range(FULL):
        for u in range(SPLIT):
            back[0, pl.ds(u * FULL + v, C, stride=ROWS), :] = jnp.maximum(
                e_gain * enc_hat_of(v, u) + e_bias, 0.0
            )
    enc_flat[...] = back[0].astype(jnp.bfloat16)

    lanes8 = lanes_of((8, LANES))
    per_peer = UNIT // n_dp

    def send_unit(n, left, right):
        for a in range(3):
            for b in range(3):
                acc = jnp.zeros((WIDE, C), jnp.float32)
                for u in range(SPLIT):
                    acc = acc + dot_t(left(u), right(u, a, b))
                t = 3 * a + b
                grads[n, t * WIDE : (t + 1) * WIDE, 0:C] = acc * grad_scale
        for p in range(n_dp):
            block = grads[n, pl.ds(p * per_peer, 8, stride=4), :]
            for g in range(1, 4):
                rows = grads[n, pl.ds(p * per_peer + g, 8, stride=4), :]
                block = jnp.where(lanes8 < 32 * g, block, pltpu.roll(rows, 32 * g, 1))
            terms[n, p] = block.astype(SEND)

        def start(i, carry):
            far_copy(n, i).start()
            return carry

        lax.fori_loop(1, n_dp, start, 0)

    def far_copy(n, i):
        peer = lax.rem(me + i * ORDER, n_dp)
        return pltpu.make_async_remote_copy(
            src_ref=terms.at[n, peer], dst_ref=arrived.at[n, me],
            send_sem=far_s.at[n], recv_sem=far_r.at[n], device_id={DP: peer},
        )

    def far_all(n):
        return pltpu.make_async_remote_copy(
            src_ref=terms.at[n, pl.ds(0, n_dp - 1)], dst_ref=arrived.at[n, pl.ds(0, n_dp - 1)],
            send_sem=far_s.at[n], recv_sem=far_r.at[n], device_id={DP: along(1)},
        )

    heard(3)
    halo_arrived(1)
    send_unit(1, lambda u: c3[u], lambda u, a, b: xd[u + b, :, lane(a, FULL)])

    gain = e_gain * e_scale
    for i in range(1, n_space):
        skip_arrival(i).wait_recv()
    skip_own.wait()
    for j in range(n_space):
        shift = gain * (unpack(stat_got[0, j], 16)[0] * (1.0 / cells) - e_mean) + e_bias
        for w in range(SPLIT):
            at = lane(1 + SPLIT * j + w)
            for u in range(4):
                act = jnp.maximum(gain * xs[u, :, at].astype(jnp.float32) + shift, 0.0)
                if u == 0:
                    act = jnp.where(slab > 0, act, 0.0)
                if u == 3:
                    act = jnp.where(slab < last, act, 0.0)
                xs[u, :, at] = act.astype(jnp.bfloat16)

    first, second = zero, zero
    for u in range(SPLIT):
        for q in range(0, FULL, chunk):
            acc = jnp.zeros((WIDE, chunk * LANES), jnp.float32)
            for a in range(3):
                for b in range(3):
                    at = lane(q + a, chunk)
                    joined = jnp.concatenate([xd[u + b, :, at], xs[u + b, :, at]], axis=0)
                    acc = acc + dot(dec_w[3 * a + b], joined)
            for r in range(chunk):
                row = merge_taps(acc[:, lane(r)])
                dec_pre[u, :, lane(q + r)] = row
                first = first + row
                second = second + row * row
    packed = send_stats(2, first, second)
    own_mean = unpack(packed, 16)[0] * (1.0 / cells)
    for u in range(SPLIT):
        for v in range(FULL):
            dec_raw[u, :, lane(v)] = (dec_pre[u, :, lane(v)] - own_mean).astype(jnp.bfloat16)

    def hand(k):
        src, dst, step = ((enc_flat, enc_out, 1), (dec_raw, dec_got, -1), (coef_send, coef_got, -1))[k]
        return pltpu.make_async_remote_copy(
            src_ref=src, dst_ref=dst, send_sem=hand_s.at[k], recv_sem=hand_r.at[k],
            device_id={SECTION: level + step},
        )

    @pl.when(level > 0)
    def _():
        hand(1).start()

    @pl.when(level < n_section - 1)
    def _():
        hand(0).start()

    g_mean, gh_mean = all_stats(1)
    for u in range(SPLIT):
        for v in range(FULL):
            hat = enc_hat_of(v, u)
            row = (gated_of(v, u, hat) - g_mean - hat * gh_mean) * e_scale
            row = row.astype(jnp.bfloat16).astype(jnp.float32)
            e3[u, :, lane(v)] = gather_taps(row)
    send_unit(0, lambda u: e3[u], lambda u, a, b: x[u + a, :, lane(b, FULL)])
    send_unit(2, lambda u: c3[u], lambda u, a, b: xs[u + b, :, lane(a, FULL)])

    d_mean, d_square = all_stats(2)
    d_gain = d_gain * lax.rsqrt(d_square - d_mean * d_mean + EPS)
    coef_send[...] = pack_pair(d_gain, d_gain * (own_mean - d_mean) + d_bias)

    @pl.when(level > 0)
    def _():
        hand(2).start()

    @pl.when(level == 0)
    def _():
        enc_out[...] = jnp.zeros(enc_out.shape, enc_out.dtype)

    for n in (1, 0, 2):
        far_all(n).wait_recv()
        arrived[n, me] = terms[n, me]
        sums = [arrived[n, p].astype(jnp.float32) for p in range(n_dp)]
        while len(sums) > 1:
            sums = [a + b for a, b in zip(sums[::2], sums[1::2])]
        near_send[n] = sums[0]

    def near_copy(i):
        return pltpu.make_async_remote_copy(
            src_ref=near_send, dst_ref=near_got.at[i - 1],
            send_sem=near_s.at[i - 1], recv_sem=near_r.at[i - 1],
            device_id={SPACE: lax.rem(slab + i, n_space)},
        )

    for i in range(1, n_space):
        near_copy(i).start()

    @pl.when(level < n_section - 1)
    def _():
        hand(1).wait_recv()
        hand(2).wait_recv()
        scale, shift = unpack(coef_got[...], 1)
        for u in range(SPLIT):
            for v in range(FULL):
                back[1, pl.ds(v * SPLIT + u, C, stride=ROWS), :] = jnp.maximum(
                    scale * dec_got[u, :, lane(v)].astype(jnp.float32) + shift, 0.0
                )
        dec_out[...] = back[1].astype(jnp.bfloat16)

    @pl.when(level == n_section - 1)
    def _():
        dec_out[...] = jnp.zeros(dec_out.shape, dec_out.dtype)

    acc = near_send[...]
    for i in range(1, n_space):
        near_copy(i).wait_recv()
        acc = acc + near_got[i - 1]
    total[...] = acc

    @pl.when(level > 0)
    def _():
        hand(0).wait_recv()
        hand(1).wait_send()
        hand(2).wait_send()

    @pl.when(level < n_section - 1)
    def _():
        hand(0).wait_send()

    @pl.when(slab < last)
    def _():
        for k in range(2):
            halo(k, True).wait_send()

    @pl.when(slab > 0)
    def _():
        for k in range(2):
            halo(k, False).wait_send()

    for i in range(1, n_space):
        for n in range(3):
            stat_copy(n, i).wait_send()
        cot_copy(i).wait_send()
        skip_copy(i).wait_send()
        near_copy(i).wait_send()
    for n in range(3):
        far_all(n).wait_send()


def finish(n_space, enc_in, dec_in, sums, enc_hbm, dec_hbm, enc_grad, dec_grad, sems):
    slab = lax.axis_index(SPACE)
    copies = [
        pltpu.make_async_copy(enc_in, enc_hbm, sems.at[0]),
        pltpu.make_async_copy(dec_in, dec_hbm, sems.at[1]),
    ]
    for copy in copies:
        copy.start()

    def part(rows, out):
        flat = jnp.concatenate(rows, axis=1)
        width = out.shape[1]
        mine = flat[:, 0:width]
        for j in range(1, n_space):
            mine = jnp.where(slab == j, flat[:, j * width : (j + 1) * width], mine)
        out[...] = mine

    part([sums[0, r : r + 1, :] for r in range(7)], enc_grad)
    own, skip = sums[1], sums[2]
    group = lanes_of((8, LANES)) // C
    even = jnp.where(
        group == 0, own,
        jnp.where(
            group == 1, pltpu.roll(skip, 32, 1),
            jnp.where(group == 2, pltpu.roll(own, 32, 1), pltpu.roll(skip, 64, 1)),
        ),
    )
    odd = jnp.where(
        group == 0, pltpu.roll(own, 64, 1),
        jnp.where(
            group == 1, pltpu.roll(skip, 96, 1),
            jnp.where(group == 2, pltpu.roll(own, 96, 1), skip),
        ),
    )
    rows = []
    for r in range(7):
        rows += [even[r : r + 1, :], odd[r : r + 1, :]]
    part(rows, dec_grad)
    for copy in copies:
        copy.wait()


def body(
    enc_input, dec_input, dec_cotangent, deep_cotangent,
    enc_weight, dec_weight, enc_gain, enc_bias, dec_gain, dec_bias,
):
    n_section, n_dp, n_space = (lax.axis_size(a) for a in (SECTION, DP, SPACE))
    voxels = enc_input.shape[3] * n_space * enc_input.shape[4] * enc_input.shape[5]
    grad_scale = 1.0 / math.sqrt(n_dp * voxels)
    flat = (C * ROWS, LANES)
    vmem = pl.BlockSpec(memory_space=pltpu.VMEM)
    hbm = pl.BlockSpec(memory_space=pltpu.HBM)
    bf16, f32 = jnp.bfloat16, jnp.float32
    dma = pltpu.SemaphoreType.DMA
    others = n_space - 1
    enc_out, dec_out, total = pl.pallas_call(
        lambda *refs: kernel(n_section, n_dp, n_space, voxels, grad_scale, *refs),
        out_shape=(
            pltpu.VMEM(flat, bf16),
            pltpu.VMEM(flat, bf16),
            pltpu.VMEM((3, 8, LANES), f32),
        ),
        in_specs=[hbm] * 10,
        out_specs=(vmem, vmem, vmem),
        scratch_shapes=[
            pltpu.VMEM((4, *flat), bf16),
            pltpu.VMEM((TAPS, WIDE, C), bf16),
            pltpu.VMEM((TAPS, WIDE, 2 * C), bf16),
            pltpu.VMEM((4, 1, C), f32),
            pltpu.VMEM((4, *flat), f32),
            pltpu.VMEM((2, *flat), f32),
            pltpu.VMEM((4, C, PADDED), bf16),
            pltpu.VMEM((4, C, PADDED), bf16),
            pltpu.VMEM((4, C, PADDED), bf16),
            pltpu.VMEM((4, C, PADDED), bf16),
            pltpu.VMEM((FULL + 2, C, PAIR), bf16),
            pltpu.VMEM((SPLIT, WIDE, RUN), bf16),
            pltpu.VMEM((4, WIDE, PADDED), bf16),
            pltpu.VMEM((SPLIT, WIDE, RUN), bf16),
            pltpu.VMEM((FULL + 2, C, PAIR), bf16),
            pltpu.VMEM((FULL, C, PAIR), bf16),
            pltpu.VMEM((FULL, C, PAIR), f32),
            pltpu.VMEM((FULL, C, PAIR), f32),
            pltpu.VMEM((SPLIT, C, RUN), f32),
            pltpu.VMEM((LANES, LANES), f32),
            pltpu.VMEM((TAPS, C, WIDE), bf16),
            pltpu.VMEM((3, 8, LANES), f32),
            pltpu.VMEM((3, n_space, 8, LANES), f32),
            pltpu.VMEM((3, UNIT + 8, LANES), f32),
            pltpu.VMEM((3, n_dp, 8, LANES), SEND),
            pltpu.VMEM((3, n_dp, 8, LANES), SEND),
            pltpu.VMEM((3, 8, LANES), f32),
            pltpu.VMEM((others, 3, 8, LANES), f32),
            pltpu.VMEM(flat, bf16),
            pltpu.VMEM((SPLIT, C, RUN), bf16),
            pltpu.VMEM((SPLIT, C, RUN), bf16),
            pltpu.VMEM((8, LANES), f32),
            pltpu.VMEM((8, LANES), f32),
            dma((10,)),
            dma((4,)), dma((4,)),
            dma((3 * others,)), dma((3 * others,)),
            dma((others,)), dma((others,)),
            dma((others,)), dma((others,)),
            dma((2,)),
            dma((3,)), dma((3,)),
            dma((3,)), dma((3,)),
            dma((others,)), dma((others,)),
            pltpu.SemaphoreType.REGULAR((4,)),
        ],
        compiler_params=pltpu.CompilerParams(
            collective_id=0, has_side_effects=True, vmem_limit_bytes=48 * 1024 * 1024
        ),
    )(
        *(
            pltpu.with_memory_space_constraint(array, pltpu.HBM)
            for array in (
                enc_input.reshape(flat), dec_input.reshape(flat), dec_cotangent.reshape(flat),
                deep_cotangent.reshape(flat), enc_weight.reshape(TAPS, WIDE, C),
                dec_weight.reshape(TAPS, WIDE, 2 * C), enc_gain, enc_bias, dec_gain, dec_bias,
            )
        )
    )
    enc_width, dec_width = UNIT * C // (n_dp * n_space), 2 * UNIT * C // (n_dp * n_space)
    enc_out, dec_out, enc_grad, dec_grad = pl.pallas_call(
        lambda *refs: finish(n_space, *refs),
        out_shape=(
            jax.ShapeDtypeStruct(flat, bf16),
            jax.ShapeDtypeStruct(flat, bf16),
            jax.ShapeDtypeStruct((1, enc_width), f32),
            jax.ShapeDtypeStruct((1, dec_width), f32),
        ),
        in_specs=[vmem] * 3,
        out_specs=(hbm, hbm, vmem, vmem),
        scratch_shapes=[dma((2,))],
        compiler_params=pltpu.CompilerParams(vmem_limit_bytes=4 * 1024 * 1024),
    )(enc_out, dec_out, total)
    return (
        enc_out.reshape(enc_input.shape), dec_out.reshape(dec_input.shape), enc_grad, dec_grad
    )


def solution(mesh):
    by_depth = P(SECTION, DP, None, SPACE, None, None)
    by_height = P(SECTION, DP, None, None, SPACE, None)
    whole3, whole1 = P(SECTION, None, None, None), P(SECTION, None)
    return jax.shard_map(
        body,
        mesh=mesh,
        in_specs=(by_depth, by_height, by_height, by_depth, whole3, whole3, *[whole1] * 4),
        out_specs=(by_depth, by_height, P(SECTION, (DP, SPACE)), P(SECTION, (DP, SPACE))),
        check_vma=False,
    )
```

```python
import math

import jax
import jax.numpy as jnp
from jax import lax
from jax.experimental import pallas as pl
from jax.experimental.pallas import tpu as pltpu
from jax.sharding import PartitionSpec as P

SPACE = "space"
DP = "dp"
SECTION = "section"

EPS = 1e-05

C = 32
LANES = 128
FULL = 8
SPLIT = 2
ROWS = FULL * SPLIT
RUN = FULL * LANES
PADDED = (FULL + 2) * LANES
PAIR = SPLIT * LANES
TAPS = 9
WIDE = 3 * C
UNIT = TAPS * WIDE
RING = 8
SEND = jnp.bfloat16


def dot(a, b):
    return jnp.dot(a, b, preferred_element_type=jnp.float32)


def dot_t(a, b):
    return lax.dot_general(a, b, (((1,), (1,)), ((), ())), preferred_element_type=jnp.float32)


def lanes_of(shape):
    return lax.broadcasted_iota(jnp.int32, shape, len(shape) - 1)


def to_right(row):
    return jnp.where(lanes_of(row.shape) == 0, 0.0, pltpu.roll(row, 1, 1))


def to_left(row):
    return jnp.where(lanes_of(row.shape) == LANES - 1, 0.0, pltpu.roll(row, LANES - 1, 1))


def gather_taps(row):
    return jnp.concatenate([to_left(row), row, to_right(row)], axis=0).astype(jnp.bfloat16)


def merge_taps(wide):
    return to_right(wide[0:C]) + wide[C : 2 * C] + to_left(wide[2 * C : 3 * C])


def pack_stats(first, second):
    lanes = lanes_of((8, LANES))
    packed = jnp.zeros((8, LANES), jnp.float32)
    for k in range(4):
        for n, whole in enumerate((first, second)):
            part = whole[8 * k : 8 * k + 8]
            for shift in (64, 32, 16):
                part = part + pltpu.roll(part, shift, 1)
            low = 32 * k + 16 * n
            packed = jnp.where((lanes >= low) & (lanes < low + 16), part, packed)
    return packed


def pack_pair(first, second):
    lanes = lanes_of((8, LANES))
    packed = jnp.zeros((8, LANES), jnp.float32)
    for k in range(4):
        for n, whole in enumerate((first, second)):
            low = 32 * k + 16 * n
            mine = (lanes >= low) & (lanes < low + 16)
            packed = jnp.where(mine, whole[8 * k : 8 * k + 8], packed)
    return packed


def unpack(packed, width):
    lanes = lanes_of((8, LANES))
    both = []
    for n in range(2):
        pieces = []
        for k in range(4):
            low = 32 * k + 16 * n
            mine = jnp.where((lanes >= low) & (lanes < low + width), packed, 0.0)
            pieces.append(jnp.sum(mine, axis=1, keepdims=True))
        both.append(jnp.concatenate(pieces, axis=0))
    return both


def kernel(
    n_section, n_dp, n_space, voxels, grad_scale,
    enc_hbm, dec_hbm, cot_hbm, deep_hbm, enc_w_hbm, dec_w_hbm, g0, g1, g2, g3,
    enc_out, dec_out, total,
    loaded, enc_w, dec_w, params,
    stage, back, x, xd, xs, xc, cot_send, c3, c3e, e3, skip_send, sg, deep, pre, dec_pre,
    prm, tr_w, wide_e, wide_d, stat_send, stat_got, grads, terms, arrived, near_send, near_got,
    enc_flat, dec_raw, dec_got, coef_send, coef_got,
    load_s, halo_s, halo_r, stat_s, stat_r, skip_s, skip_r, cot_s, cot_r, own_sem,
    hand_s, hand_r, far_s, far_r, near_s, near_r, known,
):
    me = lax.axis_index(DP)
    slab = lax.axis_index(SPACE)
    level = lax.axis_index(SECTION)
    last = n_space - 1
    cells = ROWS * LANES

    loads = [
        pltpu.make_async_copy(src, dst, load_s.at[n])
        for n, (src, dst) in enumerate(
            (
                (enc_hbm, loaded.at[0]), (cot_hbm, loaded.at[1]), (enc_w_hbm, enc_w),
                (dec_hbm, loaded.at[2]), (deep_hbm, loaded.at[3]), (dec_w_hbm, dec_w),
                (g0, params.at[0]), (g1, params.at[1]), (g2, params.at[2]), (g3, params.at[3]),
            )
        )
    ]
    for load in loads:
        load.start()

    barrier = pltpu.get_barrier_semaphore()

    ring = min(RING, n_dp)
    far, near = lax.div(me, ring), lax.rem(me, ring)

    def along(step):
        return far * ring + lax.rem(near + step + ring, ring)

    def across(step):
        return lax.rem(far + step + n_dp // ring, n_dp // ring) * ring + near

    def tell(sem, peers):
        for peer in peers:
            pl.semaphore_signal(sem, inc=1, device_id={DP: peer})

    def heard(n):
        pl.semaphore_wait(known.at[n], 2)

    for i in range(1, n_space):
        pl.semaphore_signal(barrier, inc=1, device_id={SPACE: lax.rem(slab + i, n_space)})
    tell(barrier, (along(1), along(-1), across(1), across(-1)))

    @pl.when(level > 0)
    def _():
        pl.semaphore_signal(barrier, inc=1, device_id={SECTION: level - 1})

    @pl.when(level < n_section - 1)
    def _():
        pl.semaphore_signal(barrier, inc=1, device_id={SECTION: level + 1})

    def row_of(k, r):
        return stage[k, pl.ds(r, C, stride=ROWS), :]

    def lane(r, n=1):
        return slice(r * LANES, (r + n) * LANES)

    inner = lane(1, FULL)

    for ref in (x, xd, xs, xc):
        ref[:, :, lane(0)] = jnp.zeros((4, C, LANES), ref.dtype)
        ref[:, :, lane(FULL + 1)] = jnp.zeros((4, C, LANES), ref.dtype)
    c3e[:, :, lane(0)] = jnp.zeros((4, WIDE, LANES), c3e.dtype)
    c3e[:, :, lane(FULL + 1)] = jnp.zeros((4, WIDE, LANES), c3e.dtype)
    for ref in (skip_send, cot_send):
        ref[0] = jnp.zeros((C, PAIR), ref.dtype)
        ref[FULL + 1] = jnp.zeros((C, PAIR), ref.dtype)

    @pl.when(slab == 0)
    def _():
        x[0] = jnp.zeros((C, PADDED), x.dtype)
        xd[0] = jnp.zeros((C, PADDED), xd.dtype)
        xc[0] = jnp.zeros((C, PADDED), xc.dtype)
        xs[0] = jnp.zeros((C, PADDED), xs.dtype)

    @pl.when(slab == last)
    def _():
        x[3] = jnp.zeros((C, PADDED), x.dtype)
        xd[3] = jnp.zeros((C, PADDED), xd.dtype)
        xc[3] = jnp.zeros((C, PADDED), xc.dtype)
        xs[3] = jnp.zeros((C, PADDED), xs.dtype)

    loads[0].wait()
    stage[0] = loaded[0].astype(jnp.float32)
    for u in range(SPLIT):
        for v in range(FULL):
            x[1 + u, :, lane(1 + v)] = row_of(0, u * FULL + v).astype(jnp.bfloat16)
    loads[1].wait()
    stage[1] = loaded[1].astype(jnp.float32)
    for u in range(SPLIT):
        for v in range(FULL):
            cot_send[1 + v, :, lane(u)] = row_of(1, v * SPLIT + u).astype(jnp.bfloat16)
    loads[3].wait()
    stage[2] = loaded[2].astype(jnp.float32)
    for u in range(SPLIT):
        for v in range(FULL):
            xd[1 + u, :, lane(1 + v)] = row_of(2, v * SPLIT + u).astype(jnp.bfloat16)

    def halo(k, up):
        src_u, dst_u, peer = (2, 0, slab + 1) if up else (1, 3, slab - 1)
        ref = (x, xd)[k]
        n = 2 * k + (0 if up else 1)
        return pltpu.make_async_remote_copy(
            src_ref=ref.at[src_u, :, inner], dst_ref=ref.at[dst_u, :, inner],
            send_sem=halo_s.at[n], recv_sem=halo_r.at[n], device_id={SPACE: peer},
        )

    def halo_start(k):
        @pl.when(slab < last)
        def _():
            halo(k, True).start()

        @pl.when(slab > 0)
        def _():
            halo(k, False).start()

    def halo_arrived(k):
        @pl.when(slab > 0)
        def _():
            halo(k, True).wait_recv()

        @pl.when(slab < last)
        def _():
            halo(k, False).wait_recv()

    def regroup(sender, receiver, send_sem, recv_sem, own):
        def refs(source, target, first, count):
            at = pl.multiple_of((1 + source * SPLIT) * LANES, LANES)
            return (
                sender.at[pl.ds(target * SPLIT + first, count)],
                receiver.at[pl.ds(first, count), :, pl.ds(at, PAIR)],
            )

        def remote(i, peer, source, target, first, count):
            src, dst = refs(source, target, first, count)
            return pltpu.make_async_remote_copy(
                src_ref=src, dst_ref=dst, send_sem=send_sem.at[i - 1],
                recv_sem=recv_sem.at[i - 1], device_id={SPACE: peer},
            )

        def copies(act):
            for i in range(1, n_space):
                peer = lax.rem(slab + i, n_space)
                by_end(peer, lambda *cut: act(remote(i, peer, slab, peer, *cut)))

        def arrivals():
            for i in range(1, n_space):
                peer = lax.rem(slab - i + n_space, n_space)
                by_end(slab, lambda *cut: remote(i, peer, peer, slab, *cut).wait_recv())

        return copies, arrivals, pltpu.make_async_copy(*refs(slab, slab, 0, SPLIT + 2), own)

    def by_end(target, act):
        @pl.when(target == 0)
        def _():
            act(1, SPLIT + 1)

        @pl.when(target == last)
        def _():
            act(0, SPLIT + 1)

        @pl.when((target > 0) & (target < last))
        def _():
            act(0, SPLIT + 2)

    cot_copies, cot_arrivals, cot_own = regroup(cot_send, xc, cot_s, cot_r, own_sem.at[0])
    skip_copies, skip_arrivals, skip_own = regroup(skip_send, xs, skip_s, skip_r, own_sem.at[1])

    pl.semaphore_wait(
        barrier, 4 + n_space - 1 + lax.min(level, 1) + lax.min(n_section - 1 - level, 1)
    )
    halo_start(0)
    cot_copies(lambda copy: copy.start())
    cot_own.start()
    halo_start(1)
    tell(known.at[0], (along(1), along(-1)))

    for n in (6, 7, 8, 9):
        loads[n].wait()
    prm[...] = jnp.zeros((LANES, LANES), jnp.float32)
    for n in range(4):
        prm[n : n + 1, 0:C] = params[n]
    columns = prm[...].T
    e_gain, e_bias = columns[0:C, 0:1], columns[0:C, 1:2]
    d_gain, d_bias = columns[0:C, 2:3], columns[0:C, 3:4]
    pick = (
        lax.broadcasted_iota(jnp.int32, (C, 2 * C), 1)
        == lax.broadcasted_iota(jnp.int32, (C, 2 * C), 0) + C
    ).astype(jnp.bfloat16)
    loads[5].wait()
    for t in range(TAPS):
        tr_w[t] = dot_t(pick, dec_w[t]).astype(jnp.bfloat16)
    loads[2].wait()
    for k in range(3):
        wide_e[k] = jnp.concatenate([enc_w[3 * k + b] for b in range(3)], axis=1)
        wide_d[k] = jnp.concatenate([dec_w[3 * a + k] for a in range(3)], axis=1)
    loads[4].wait()
    stage[3] = loaded[3].astype(jnp.float32)
    for u in range(SPLIT):
        for v in range(FULL):
            c3[u, :, lane(v)] = gather_taps(row_of(1, v * SPLIT + u))
            deep[v, :, lane(u)] = row_of(3, u * FULL + v)
    heard(0)
    tell(known.at[1], (along(2), along(-2)))

    zero = jnp.zeros((C, LANES), jnp.float32)
    chunk = 2

    halo_arrived(0)
    first, second = zero, zero
    for u in range(SPLIT):
        for q in range(0, FULL, chunk):
            acc = jnp.zeros((WIDE, chunk * LANES), jnp.float32)
            for a in range(3):
                three = [x[u + a, :, lane(q + b, chunk)] for b in range(3)]
                acc = acc + dot(wide_e[a], jnp.concatenate(three, axis=0))
            for r in range(chunk):
                row = merge_taps(acc[:, lane(r)])
                pre[q + r, :, lane(u)] = row
                first = first + row
                second = second + row * row

    def stat_copy(n, i):
        k = n * (n_space - 1) + i - 1
        return pltpu.make_async_remote_copy(
            src_ref=stat_send.at[n], dst_ref=stat_got.at[n, slab],
            send_sem=stat_s.at[k], recv_sem=stat_r.at[k],
            device_id={SPACE: lax.rem(slab + i, n_space)},
        )

    def stat_arrival(n, i):
        k = n * (n_space - 1) + i - 1
        peer = lax.rem(slab - i + n_space, n_space)
        return pltpu.make_async_remote_copy(
            src_ref=stat_send.at[n], dst_ref=stat_got.at[n, peer],
            send_sem=stat_s.at[k], recv_sem=stat_r.at[k], device_id={SPACE: peer},
        )

    def send_stats(n, first, second):
        packed = pack_stats(first, second)
        stat_send[n] = packed
        for i in range(1, n_space):
            stat_copy(n, i).start()
        stat_got[n, slab] = packed
        return packed

    def all_stats(n):
        for i in range(1, n_space):
            stat_arrival(n, i).wait_recv()
        packed = stat_got[n, 0]
        for j in range(1, n_space):
            packed = packed + stat_got[n, j]
        one, two = unpack(packed, 16)
        return one * (1.0 / voxels), two * (1.0 / voxels)

    packed = send_stats(0, first, second)
    own_mean = unpack(packed, 16)[0] * (1.0 / cells)
    for v in range(FULL):
        for u in range(SPLIT):
            skip_send[1 + v, :, lane(u)] = (pre[v, :, lane(u)] - own_mean).astype(jnp.bfloat16)
    skip_copies(lambda copy: copy.start())
    skip_own.start()
    heard(1)
    tell(known.at[2], (across(1), across(-1)))

    cot_arrivals()
    cot_own.wait()
    for u in range(4):
        for v in range(FULL):
            c3e[u, :, lane(1 + v)] = gather_taps(xc[u, :, lane(1 + v)].astype(jnp.float32))
    for u in range(SPLIT):
        for q in range(0, FULL, chunk):
            acc = jnp.zeros((C, chunk * LANES), jnp.float32)
            for a in range(3):
                for b in range(3):
                    acc = acc + dot(tr_w[3 * a + b], c3e[u + 2 - a, :, lane(q + 2 - b, chunk)])
            for r in range(chunk):
                sg[q + r, :, lane(u)] = acc[:, lane(r)].astype(jnp.bfloat16)

    heard(2)
    tell(known.at[3], (across(1), across(-1)))

    e_mean, e_square = all_stats(0)
    e_scale = lax.rsqrt(e_square - e_mean * e_mean + EPS)

    def enc_hat_of(v, u):
        return (pre[v, :, lane(u)] - e_mean) * e_scale

    def gated_of(v, u, hat):
        upstream = sg[v, :, lane(u)].astype(jnp.float32) + deep[v, :, lane(u)]
        return jnp.where(e_gain * hat + e_bias > 0, upstream, 0.0) * e_gain

    first, second = zero, zero
    for v in range(FULL):
        for u in range(SPLIT):
            hat = enc_hat_of(v, u)
            gated = gated_of(v, u, hat)
            first = first + gated
            second = second + gated * hat
    send_stats(1, first, second)
    for v in range(FULL):
        for u in range(SPLIT):
            back[0, pl.ds(u * FULL + v, C, stride=ROWS), :] = jnp.maximum(
                e_gain * enc_hat_of(v, u) + e_bias, 0.0
            )
    enc_flat[...] = back[0].astype(jnp.bfloat16)

    lanes8 = lanes_of((8, LANES))
    per_peer = UNIT // n_dp

    def send_unit(n, left, right):
        for a in range(3):
            for b in range(3):
                acc = jnp.zeros((WIDE, C), jnp.float32)
                for u in range(SPLIT):
                    acc = acc + dot_t(left(u), right(u, a, b))
                t = 3 * a + b
                grads[n, t * WIDE : (t + 1) * WIDE, 0:C] = acc * grad_scale
        for p in range(n_dp):
            block = grads[n, pl.ds(p * per_peer, 8, stride=4), :]
            for g in range(1, 4):
                rows = grads[n, pl.ds(p * per_peer + g, 8, stride=4), :]
                block = jnp.where(lanes8 < 32 * g, block, pltpu.roll(rows, 32 * g, 1))
            terms[n, p] = block.astype(SEND)

        for dx, dz in hops:
            far_copy(n, dx, dz).start()

    columns_of = n_dp // ring

    def steps(d, n):
        return min(d, n - d)

    hops = sorted(
        ((dx, dz) for dx in range(columns_of) for dz in range(ring) if dx or dz),
        key=lambda hop: (-steps(hop[0], columns_of) - steps(hop[1], ring), hop[0] * 3 % 4, hop[1] * 5 % 8),
    )

    def far_copy(n, dx, dz):
        peer = lax.rem(far + dx, columns_of) * ring + lax.rem(near + dz, ring)
        return pltpu.make_async_remote_copy(
            src_ref=terms.at[n, peer], dst_ref=arrived.at[n, me],
            send_sem=far_s.at[n], recv_sem=far_r.at[n], device_id={DP: peer},
        )

    def far_all(n):
        return pltpu.make_async_remote_copy(
            src_ref=terms.at[n, pl.ds(0, n_dp - 1)], dst_ref=arrived.at[n, pl.ds(0, n_dp - 1)],
            send_sem=far_s.at[n], recv_sem=far_r.at[n], device_id={DP: along(1)},
        )

    heard(3)
    halo_arrived(1)
    send_unit(1, lambda u: c3[u], lambda u, a, b: xd[u + b, :, lane(a, FULL)])

    gain = e_gain * e_scale
    skip_arrivals()
    skip_own.wait()
    for j in range(n_space):
        shift = gain * (unpack(stat_got[0, j], 16)[0] * (1.0 / cells) - e_mean) + e_bias
        for w in range(SPLIT):
            at = lane(1 + SPLIT * j + w)
            for u in range(4):
                act = jnp.maximum(gain * xs[u, :, at].astype(jnp.float32) + shift, 0.0)
                if u == 0:
                    act = jnp.where(slab > 0, act, 0.0)
                if u == 3:
                    act = jnp.where(slab < last, act, 0.0)
                xs[u, :, at] = act.astype(jnp.bfloat16)

    first, second = zero, zero
    for u in range(SPLIT):
        for q in range(0, FULL, chunk):
            acc = jnp.zeros((WIDE, chunk * LANES), jnp.float32)
            for b in range(3):
                three = []
                for a in range(3):
                    at = lane(q + a, chunk)
                    three += [xd[u + b, :, at], xs[u + b, :, at]]
                acc = acc + dot(wide_d[b], jnp.concatenate(three, axis=0))
            for r in range(chunk):
                row = merge_taps(acc[:, lane(r)])
                dec_pre[u, :, lane(q + r)] = row
                first = first + row
                second = second + row * row
    packed = send_stats(2, first, second)
    own_mean = unpack(packed, 16)[0] * (1.0 / cells)
    for u in range(SPLIT):
        for v in range(FULL):
            dec_raw[u, :, lane(v)] = (dec_pre[u, :, lane(v)] - own_mean).astype(jnp.bfloat16)

    def hand(k):
        src, dst, step = ((enc_flat, enc_out, 1), (dec_raw, dec_got, -1), (coef_send, coef_got, -1))[k]
        return pltpu.make_async_remote_copy(
            src_ref=src, dst_ref=dst, send_sem=hand_s.at[k], recv_sem=hand_r.at[k],
            device_id={SECTION: level + step},
        )

    @pl.when(level > 0)
    def _():
        hand(1).start()

    @pl.when(level < n_section - 1)
    def _():
        hand(0).start()

    g_mean, gh_mean = all_stats(1)
    for u in range(SPLIT):
        for v in range(FULL):
            hat = enc_hat_of(v, u)
            row = (gated_of(v, u, hat) - g_mean - hat * gh_mean) * e_scale
            row = row.astype(jnp.bfloat16).astype(jnp.float32)
            e3[u, :, lane(v)] = gather_taps(row)
    send_unit(0, lambda u: e3[u], lambda u, a, b: x[u + a, :, lane(b, FULL)])
    send_unit(2, lambda u: c3[u], lambda u, a, b: xs[u + b, :, lane(a, FULL)])

    d_mean, d_square = all_stats(2)
    d_gain = d_gain * lax.rsqrt(d_square - d_mean * d_mean + EPS)
    coef_send[...] = pack_pair(d_gain, d_gain * (own_mean - d_mean) + d_bias)

    @pl.when(level > 0)
    def _():
        hand(2).start()

    @pl.when(level == 0)
    def _():
        enc_out[...] = jnp.zeros(enc_out.shape, enc_out.dtype)

    for n in (1, 0, 2):
        far_all(n).wait_recv()
        arrived[n, me] = terms[n, me]
        sums = [arrived[n, p].astype(jnp.float32) for p in range(n_dp)]
        while len(sums) > 1:
            sums = [a + b for a, b in zip(sums[::2], sums[1::2])]
        near_send[n] = sums[0]

    def near_copy(i):
        return pltpu.make_async_remote_copy(
            src_ref=near_send, dst_ref=near_got.at[i - 1],
            send_sem=near_s.at[i - 1], recv_sem=near_r.at[i - 1],
            device_id={SPACE: lax.rem(slab + i, n_space)},
        )

    for i in range(1, n_space):
        near_copy(i).start()

    @pl.when(level < n_section - 1)
    def _():
        hand(1).wait_recv()
        hand(2).wait_recv()
        scale, shift = unpack(coef_got[...], 1)
        for u in range(SPLIT):
            for v in range(FULL):
                back[1, pl.ds(v * SPLIT + u, C, stride=ROWS), :] = jnp.maximum(
                    scale * dec_got[u, :, lane(v)].astype(jnp.float32) + shift, 0.0
                )
        dec_out[...] = back[1].astype(jnp.bfloat16)

    @pl.when(level == n_section - 1)
    def _():
        dec_out[...] = jnp.zeros(dec_out.shape, dec_out.dtype)

    acc = near_send[...]
    for i in range(1, n_space):
        near_copy(i).wait_recv()
        acc = acc + near_got[i - 1]
    total[...] = acc

    @pl.when(level > 0)
    def _():
        hand(0).wait_recv()
        hand(1).wait_send()
        hand(2).wait_send()

    @pl.when(level < n_section - 1)
    def _():
        hand(0).wait_send()

    @pl.when(slab < last)
    def _():
        for k in range(2):
            halo(k, True).wait_send()

    @pl.when(slab > 0)
    def _():
        for k in range(2):
            halo(k, False).wait_send()

    for i in range(1, n_space):
        for n in range(3):
            stat_copy(n, i).wait_send()
        near_copy(i).wait_send()
    cot_copies(lambda copy: copy.wait_send())
    skip_copies(lambda copy: copy.wait_send())
    for n in range(3):
        far_all(n).wait_send()


def finish(n_space, enc_in, dec_in, sums, enc_hbm, dec_hbm, enc_grad, dec_grad, sems):
    slab = lax.axis_index(SPACE)
    copies = [
        pltpu.make_async_copy(enc_in, enc_hbm, sems.at[0]),
        pltpu.make_async_copy(dec_in, dec_hbm, sems.at[1]),
    ]
    for copy in copies:
        copy.start()

    def part(rows, out):
        flat = jnp.concatenate(rows, axis=1)
        width = out.shape[1]
        mine = flat[:, 0:width]
        for j in range(1, n_space):
            mine = jnp.where(slab == j, flat[:, j * width : (j + 1) * width], mine)
        out[...] = mine

    part([sums[0, r : r + 1, :] for r in range(7)], enc_grad)
    own, skip = sums[1], sums[2]
    group = lanes_of((8, LANES)) // C
    even = jnp.where(
        group == 0, own,
        jnp.where(
            group == 1, pltpu.roll(skip, 32, 1),
            jnp.where(group == 2, pltpu.roll(own, 32, 1), pltpu.roll(skip, 64, 1)),
        ),
    )
    odd = jnp.where(
        group == 0, pltpu.roll(own, 64, 1),
        jnp.where(
            group == 1, pltpu.roll(skip, 96, 1),
            jnp.where(group == 2, pltpu.roll(own, 96, 1), skip),
        ),
    )
    rows = []
    for r in range(7):
        rows += [even[r : r + 1, :], odd[r : r + 1, :]]
    part(rows, dec_grad)
    for copy in copies:
        copy.wait()


def body(
    enc_input, dec_input, dec_cotangent, deep_cotangent,
    enc_weight, dec_weight, enc_gain, enc_bias, dec_gain, dec_bias,
):
    n_section, n_dp, n_space = (lax.axis_size(a) for a in (SECTION, DP, SPACE))
    voxels = enc_input.shape[3] * n_space * enc_input.shape[4] * enc_input.shape[5]
    grad_scale = 1.0 / math.sqrt(n_dp * voxels)
    flat = (C * ROWS, LANES)
    vmem = pl.BlockSpec(memory_space=pltpu.VMEM)
    hbm = pl.BlockSpec(memory_space=pltpu.HBM)
    bf16, f32 = jnp.bfloat16, jnp.float32
    dma = pltpu.SemaphoreType.DMA
    others = n_space - 1
    enc_out, dec_out, total = pl.pallas_call(
        lambda *refs: kernel(n_section, n_dp, n_space, voxels, grad_scale, *refs),
        out_shape=(
            pltpu.VMEM(flat, bf16),
            pltpu.VMEM(flat, bf16),
            pltpu.VMEM((3, 8, LANES), f32),
        ),
        in_specs=[hbm] * 10,
        out_specs=(vmem, vmem, vmem),
        scratch_shapes=[
            pltpu.VMEM((4, *flat), bf16),
            pltpu.VMEM((TAPS, WIDE, C), bf16),
            pltpu.VMEM((TAPS, WIDE, 2 * C), bf16),
            pltpu.VMEM((4, 1, C), f32),
            pltpu.VMEM((4, *flat), f32),
            pltpu.VMEM((2, *flat), f32),
            pltpu.VMEM((4, C, PADDED), bf16),
            pltpu.VMEM((4, C, PADDED), bf16),
            pltpu.VMEM((4, C, PADDED), bf16),
            pltpu.VMEM((4, C, PADDED), bf16),
            pltpu.VMEM((FULL + 2, C, PAIR), bf16),
            pltpu.VMEM((SPLIT, WIDE, RUN), bf16),
            pltpu.VMEM((4, WIDE, PADDED), bf16),
            pltpu.VMEM((SPLIT, WIDE, RUN), bf16),
            pltpu.VMEM((FULL + 2, C, PAIR), bf16),
            pltpu.VMEM((FULL, C, PAIR), bf16),
            pltpu.VMEM((FULL, C, PAIR), f32),
            pltpu.VMEM((FULL, C, PAIR), f32),
            pltpu.VMEM((SPLIT, C, RUN), f32),
            pltpu.VMEM((LANES, LANES), f32),
            pltpu.VMEM((TAPS, C, WIDE), bf16),
            pltpu.VMEM((3, WIDE, 3 * C), bf16),
            pltpu.VMEM((3, WIDE, 6 * C), bf16),
            pltpu.VMEM((3, 8, LANES), f32),
            pltpu.VMEM((3, n_space, 8, LANES), f32),
            pltpu.VMEM((3, UNIT + 8, LANES), f32),
            pltpu.VMEM((3, n_dp, 8, LANES), SEND),
            pltpu.VMEM((3, n_dp, 8, LANES), SEND),
            pltpu.VMEM((3, 8, LANES), f32),
            pltpu.VMEM((others, 3, 8, LANES), f32),
            pltpu.VMEM(flat, bf16),
            pltpu.VMEM((SPLIT, C, RUN), bf16),
            pltpu.VMEM((SPLIT, C, RUN), bf16),
            pltpu.VMEM((8, LANES), f32),
            pltpu.VMEM((8, LANES), f32),
            dma((10,)),
            dma((4,)), dma((4,)),
            dma((3 * others,)), dma((3 * others,)),
            dma((others,)), dma((others,)),
            dma((others,)), dma((others,)),
            dma((2,)),
            dma((3,)), dma((3,)),
            dma((3,)), dma((3,)),
            dma((others,)), dma((others,)),
            pltpu.SemaphoreType.REGULAR((4,)),
        ],
        compiler_params=pltpu.CompilerParams(
            collective_id=0, has_side_effects=True, vmem_limit_bytes=48 * 1024 * 1024
        ),
    )(
        *(
            pltpu.with_memory_space_constraint(array, pltpu.HBM)
            for array in (
                enc_input.reshape(flat), dec_input.reshape(flat), dec_cotangent.reshape(flat),
                deep_cotangent.reshape(flat), enc_weight.reshape(TAPS, WIDE, C),
                dec_weight.reshape(TAPS, WIDE, 2 * C), enc_gain, enc_bias, dec_gain, dec_bias,
            )
        )
    )
    enc_width, dec_width = UNIT * C // (n_dp * n_space), 2 * UNIT * C // (n_dp * n_space)
    enc_out, dec_out, enc_grad, dec_grad = pl.pallas_call(
        lambda *refs: finish(n_space, *refs),
        out_shape=(
            jax.ShapeDtypeStruct(flat, bf16),
            jax.ShapeDtypeStruct(flat, bf16),
            jax.ShapeDtypeStruct((1, enc_width), f32),
            jax.ShapeDtypeStruct((1, dec_width), f32),
        ),
        in_specs=[vmem] * 3,
        out_specs=(hbm, hbm, vmem, vmem),
        scratch_shapes=[dma((2,))],
        compiler_params=pltpu.CompilerParams(vmem_limit_bytes=4 * 1024 * 1024),
    )(enc_out, dec_out, total)
    return (
        enc_out.reshape(enc_input.shape), dec_out.reshape(dec_input.shape), enc_grad, dec_grad
    )


def solution(mesh):
    by_depth = P(SECTION, DP, None, SPACE, None, None)
    by_height = P(SECTION, DP, None, None, SPACE, None)
    whole3, whole1 = P(SECTION, None, None, None), P(SECTION, None)
    return jax.shard_map(
        body,
        mesh=mesh,
        in_specs=(by_depth, by_height, by_height, by_depth, whole3, whole3, *[whole1] * 4),
        out_specs=(by_depth, by_height, P(SECTION, (DP, SPACE)), P(SECTION, (DP, SPACE))),
        check_vma=False,
    )
```

```python
import math

import jax
import jax.numpy as jnp
from jax import lax
from jax.experimental import pallas as pl
from jax.experimental.pallas import tpu as pltpu
from jax.sharding import PartitionSpec as P

SPACE = "space"
DP = "dp"
SECTION = "section"

EPS = 1e-05

C = 32
LANES = 128
FULL = 8
SPLIT = 2
ROWS = FULL * SPLIT
RUN = FULL * LANES
PADDED = (FULL + 2) * LANES
PAIR = SPLIT * LANES
TAPS = 9
WIDE = 3 * C
UNIT = TAPS * WIDE
RING = 8
SEND = jnp.bfloat16


def dot(a, b):
    return jnp.dot(a, b, preferred_element_type=jnp.float32)


def dot_t(a, b):
    return lax.dot_general(a, b, (((1,), (1,)), ((), ())), preferred_element_type=jnp.float32)


def lanes_of(shape):
    return lax.broadcasted_iota(jnp.int32, shape, len(shape) - 1)


def to_right(row):
    return jnp.where(lanes_of(row.shape) == 0, 0.0, pltpu.roll(row, 1, 1))


def to_left(row):
    return jnp.where(lanes_of(row.shape) == LANES - 1, 0.0, pltpu.roll(row, LANES - 1, 1))


def gather_taps(row):
    return jnp.concatenate([to_left(row), row, to_right(row)], axis=0).astype(jnp.bfloat16)


def merge_taps(wide):
    return to_right(wide[0:C]) + wide[C : 2 * C] + to_left(wide[2 * C : 3 * C])


def pack_stats(first, second):
    lanes = lanes_of((8, LANES))
    packed = jnp.zeros((8, LANES), jnp.float32)
    for k in range(4):
        for n, whole in enumerate((first, second)):
            part = whole[8 * k : 8 * k + 8]
            for shift in (64, 32, 16):
                part = part + pltpu.roll(part, shift, 1)
            low = 32 * k + 16 * n
            packed = jnp.where((lanes >= low) & (lanes < low + 16), part, packed)
    return packed


def pack_pair(first, second):
    lanes = lanes_of((8, LANES))
    packed = jnp.zeros((8, LANES), jnp.float32)
    for k in range(4):
        for n, whole in enumerate((first, second)):
            low = 32 * k + 16 * n
            mine = (lanes >= low) & (lanes < low + 16)
            packed = jnp.where(mine, whole[8 * k : 8 * k + 8], packed)
    return packed


def unpack(packed, width):
    lanes = lanes_of((8, LANES))
    both = []
    for n in range(2):
        pieces = []
        for k in range(4):
            low = 32 * k + 16 * n
            mine = jnp.where((lanes >= low) & (lanes < low + width), packed, 0.0)
            pieces.append(jnp.sum(mine, axis=1, keepdims=True))
        both.append(jnp.concatenate(pieces, axis=0))
    return both


def kernel(
    n_section, n_dp, n_space, voxels, grad_scale,
    enc_hbm, dec_hbm, cot_hbm, deep_hbm, enc_w_hbm, dec_w_hbm, g0, g1, g2, g3,
    enc_out, dec_out, total,
    loaded, enc_w, dec_w, params,
    stage, back, x, xd, xs, xc, cot_send, c3, c3e, e3, skip_send, sg, deep, pre, dec_pre,
    prm, tr_w, wide_e, wide_d, stat_send, stat_got, grads, terms, arrived, near_send, near_got,
    enc_flat, dec_raw, dec_got, coef_send, coef_got,
    load_s, halo_s, halo_r, stat_s, stat_r, skip_s, skip_r, cot_s, cot_r, own_sem,
    hand_s, hand_r, far_s, far_r, near_s, near_r, known,
):
    me = lax.axis_index(DP)
    slab = lax.axis_index(SPACE)
    level = lax.axis_index(SECTION)
    last = n_space - 1
    cells = ROWS * LANES

    loads = [
        pltpu.make_async_copy(src, dst, load_s.at[n])
        for n, (src, dst) in enumerate(
            (
                (enc_hbm, loaded.at[0]), (cot_hbm, loaded.at[1]), (enc_w_hbm, enc_w),
                (dec_hbm, loaded.at[2]), (deep_hbm, loaded.at[3]), (dec_w_hbm, dec_w),
                (g0, params.at[0]), (g1, params.at[1]), (g2, params.at[2]), (g3, params.at[3]),
            )
        )
    ]
    for load in loads:
        load.start()

    barrier = pltpu.get_barrier_semaphore()

    ring = min(RING, n_dp)
    far, near = lax.div(me, ring), lax.rem(me, ring)

    def along(step):
        return far * ring + lax.rem(near + step + ring, ring)

    def across(step):
        return lax.rem(far + step + n_dp // ring, n_dp // ring) * ring + near

    def tell(sem, peers):
        for peer in peers:
            pl.semaphore_signal(sem, inc=1, device_id={DP: peer})

    def heard(n):
        pl.semaphore_wait(known.at[n], 2)

    for i in range(1, n_space):
        pl.semaphore_signal(barrier, inc=1, device_id={SPACE: lax.rem(slab + i, n_space)})
    tell(barrier, (along(1), along(-1), across(1), across(-1)))

    @pl.when(level > 0)
    def _():
        pl.semaphore_signal(barrier, inc=1, device_id={SECTION: level - 1})

    @pl.when(level < n_section - 1)
    def _():
        pl.semaphore_signal(barrier, inc=1, device_id={SECTION: level + 1})

    def row_of(k, r):
        return stage[k, pl.ds(r, C, stride=ROWS), :]

    def lane(r, n=1):
        return slice(r * LANES, (r + n) * LANES)

    inner = lane(1, FULL)

    for ref in (x, xd, xs, xc):
        ref[:, :, lane(0)] = jnp.zeros((4, C, LANES), ref.dtype)
        ref[:, :, lane(FULL + 1)] = jnp.zeros((4, C, LANES), ref.dtype)
    c3e[:, :, lane(0)] = jnp.zeros((4, WIDE, LANES), c3e.dtype)
    c3e[:, :, lane(FULL + 1)] = jnp.zeros((4, WIDE, LANES), c3e.dtype)
    for ref in (skip_send, cot_send):
        ref[0] = jnp.zeros((C, PAIR), ref.dtype)
        ref[FULL + 1] = jnp.zeros((C, PAIR), ref.dtype)

    @pl.when(slab == 0)
    def _():
        x[0] = jnp.zeros((C, PADDED), x.dtype)
        xd[0] = jnp.zeros((C, PADDED), xd.dtype)
        xc[0] = jnp.zeros((C, PADDED), xc.dtype)
        xs[0] = jnp.zeros((C, PADDED), xs.dtype)

    @pl.when(slab == last)
    def _():
        x[3] = jnp.zeros((C, PADDED), x.dtype)
        xd[3] = jnp.zeros((C, PADDED), xd.dtype)
        xc[3] = jnp.zeros((C, PADDED), xc.dtype)
        xs[3] = jnp.zeros((C, PADDED), xs.dtype)

    loads[0].wait()
    stage[0] = loaded[0].astype(jnp.float32)
    for u in range(SPLIT):
        for v in range(FULL):
            x[1 + u, :, lane(1 + v)] = row_of(0, u * FULL + v).astype(jnp.bfloat16)
    loads[1].wait()
    stage[1] = loaded[1].astype(jnp.float32)
    for u in range(SPLIT):
        for v in range(FULL):
            cot_send[1 + v, :, lane(u)] = row_of(1, v * SPLIT + u).astype(jnp.bfloat16)
    loads[3].wait()
    stage[2] = loaded[2].astype(jnp.float32)
    for u in range(SPLIT):
        for v in range(FULL):
            xd[1 + u, :, lane(1 + v)] = row_of(2, v * SPLIT + u).astype(jnp.bfloat16)

    def halo(k, up):
        src_u, dst_u, peer = (2, 0, slab + 1) if up else (1, 3, slab - 1)
        ref = (x, xd)[k]
        n = 2 * k + (0 if up else 1)
        return pltpu.make_async_remote_copy(
            src_ref=ref.at[src_u, :, inner], dst_ref=ref.at[dst_u, :, inner],
            send_sem=halo_s.at[n], recv_sem=halo_r.at[n], device_id={SPACE: peer},
        )

    def halo_start(k):
        @pl.when(slab < last)
        def _():
            halo(k, True).start()

        @pl.when(slab > 0)
        def _():
            halo(k, False).start()

    def halo_arrived(k):
        @pl.when(slab > 0)
        def _():
            halo(k, True).wait_recv()

        @pl.when(slab < last)
        def _():
            halo(k, False).wait_recv()

    def regroup(sender, receiver, send_sem, recv_sem, own):
        def refs(source, target, first, count):
            at = pl.multiple_of((1 + source * SPLIT) * LANES, LANES)
            return (
                sender.at[pl.ds(target * SPLIT + first, count)],
                receiver.at[pl.ds(first, count), :, pl.ds(at, PAIR)],
            )

        def remote(i, peer, source, target, first, count):
            src, dst = refs(source, target, first, count)
            return pltpu.make_async_remote_copy(
                src_ref=src, dst_ref=dst, send_sem=send_sem.at[i - 1],
                recv_sem=recv_sem.at[i - 1], device_id={SPACE: peer},
            )

        def copies(act):
            for i in range(1, n_space):
                peer = lax.rem(slab + i, n_space)
                by_end(peer, lambda *cut: act(remote(i, peer, slab, peer, *cut)))

        def arrivals():
            for i in range(1, n_space):
                peer = lax.rem(slab - i + n_space, n_space)
                by_end(slab, lambda *cut: remote(i, peer, peer, slab, *cut).wait_recv())

        return copies, arrivals, pltpu.make_async_copy(*refs(slab, slab, 0, SPLIT + 2), own)

    def by_end(target, act):
        @pl.when(target == 0)
        def _():
            act(1, SPLIT + 1)

        @pl.when(target == last)
        def _():
            act(0, SPLIT + 1)

        @pl.when((target > 0) & (target < last))
        def _():
            act(0, SPLIT + 2)

    cot_copies, cot_arrivals, cot_own = regroup(cot_send, xc, cot_s, cot_r, own_sem.at[0])
    skip_copies, skip_arrivals, skip_own = regroup(skip_send, xs, skip_s, skip_r, own_sem.at[1])

    pl.semaphore_wait(
        barrier, 4 + n_space - 1 + lax.min(level, 1) + lax.min(n_section - 1 - level, 1)
    )
    halo_start(0)
    cot_copies(lambda copy: copy.start())
    cot_own.start()
    halo_start(1)
    tell(known.at[0], (along(1), along(-1)))

    for n in (6, 7, 8, 9):
        loads[n].wait()
    prm[...] = jnp.zeros((LANES, LANES), jnp.float32)
    for n in range(4):
        prm[n : n + 1, 0:C] = params[n]
    columns = prm[...].T
    e_gain, e_bias = columns[0:C, 0:1], columns[0:C, 1:2]
    d_gain, d_bias = columns[0:C, 2:3], columns[0:C, 3:4]
    pick = (
        lax.broadcasted_iota(jnp.int32, (C, 2 * C), 1)
        == lax.broadcasted_iota(jnp.int32, (C, 2 * C), 0) + C
    ).astype(jnp.bfloat16)
    loads[5].wait()
    for t in range(TAPS):
        tr_w[t] = dot_t(pick, dec_w[t]).astype(jnp.bfloat16)
    loads[2].wait()
    for k in range(3):
        wide_e[k] = jnp.concatenate([enc_w[3 * k + b] for b in range(3)], axis=1)
        wide_d[k] = jnp.concatenate([dec_w[3 * a + k] for a in range(3)], axis=1)
    loads[4].wait()
    stage[3] = loaded[3].astype(jnp.float32)
    for u in range(SPLIT):
        for v in range(FULL):
            c3[u, :, lane(v)] = gather_taps(row_of(1, v * SPLIT + u))
            deep[v, :, lane(u)] = row_of(3, u * FULL + v)
    heard(0)
    tell(known.at[1], (along(2), along(-2)))

    zero = jnp.zeros((C, LANES), jnp.float32)
    chunk = 2

    halo_arrived(0)
    first, second = zero, zero
    for u in range(SPLIT):
        for q in range(0, FULL, chunk):
            acc = jnp.zeros((WIDE, chunk * LANES), jnp.float32)
            for a in range(3):
                three = [x[u + a, :, lane(q + b, chunk)] for b in range(3)]
                acc = acc + dot(wide_e[a], jnp.concatenate(three, axis=0))
            for r in range(chunk):
                row = merge_taps(acc[:, lane(r)])
                pre[q + r, :, lane(u)] = row
                first = first + row
                second = second + row * row

    def stat_copy(n, i):
        k = n * (n_space - 1) + i - 1
        return pltpu.make_async_remote_copy(
            src_ref=stat_send.at[n], dst_ref=stat_got.at[n, slab],
            send_sem=stat_s.at[k], recv_sem=stat_r.at[k],
            device_id={SPACE: lax.rem(slab + i, n_space)},
        )

    def stat_arrival(n, i):
        k = n * (n_space - 1) + i - 1
        peer = lax.rem(slab - i + n_space, n_space)
        return pltpu.make_async_remote_copy(
            src_ref=stat_send.at[n], dst_ref=stat_got.at[n, peer],
            send_sem=stat_s.at[k], recv_sem=stat_r.at[k], device_id={SPACE: peer},
        )

    def send_stats(n, first, second):
        packed = pack_stats(first, second)
        stat_send[n] = packed
        for i in range(1, n_space):
            stat_copy(n, i).start()
        stat_got[n, slab] = packed
        return packed

    def all_stats(n):
        for i in range(1, n_space):
            stat_arrival(n, i).wait_recv()
        packed = stat_got[n, 0]
        for j in range(1, n_space):
            packed = packed + stat_got[n, j]
        one, two = unpack(packed, 16)
        return one * (1.0 / voxels), two * (1.0 / voxels)

    packed = send_stats(0, first, second)
    own_mean = unpack(packed, 16)[0] * (1.0 / cells)
    for v in range(FULL):
        for u in range(SPLIT):
            skip_send[1 + v, :, lane(u)] = (pre[v, :, lane(u)] - own_mean).astype(jnp.bfloat16)
    skip_copies(lambda copy: copy.start())
    skip_own.start()
    heard(1)
    tell(known.at[2], (across(1), across(-1)))

    cot_arrivals()
    cot_own.wait()
    for u in range(4):
        for v in range(FULL):
            c3e[u, :, lane(1 + v)] = gather_taps(xc[u, :, lane(1 + v)].astype(jnp.float32))
    for u in range(SPLIT):
        for q in range(0, FULL, chunk):
            acc = jnp.zeros((C, chunk * LANES), jnp.float32)
            for a in range(3):
                for b in range(3):
                    acc = acc + dot(tr_w[3 * a + b], c3e[u + 2 - a, :, lane(q + 2 - b, chunk)])
            for r in range(chunk):
                sg[q + r, :, lane(u)] = acc[:, lane(r)].astype(jnp.bfloat16)

    heard(2)
    tell(known.at[3], (across(1), across(-1)))

    e_mean, e_square = all_stats(0)
    e_scale = lax.rsqrt(e_square - e_mean * e_mean + EPS)

    def enc_hat_of(v, u):
        return (pre[v, :, lane(u)] - e_mean) * e_scale

    def gated_of(v, u, hat):
        upstream = sg[v, :, lane(u)].astype(jnp.float32) + deep[v, :, lane(u)]
        return jnp.where(e_gain * hat + e_bias > 0, upstream, 0.0) * e_gain

    first, second = zero, zero
    for v in range(FULL):
        for u in range(SPLIT):
            hat = enc_hat_of(v, u)
            gated = gated_of(v, u, hat)
            first = first + gated
            second = second + gated * hat
    send_stats(1, first, second)
    for v in range(FULL):
        for u in range(SPLIT):
            back[0, pl.ds(u * FULL + v, C, stride=ROWS), :] = jnp.maximum(
                e_gain * enc_hat_of(v, u) + e_bias, 0.0
            )
    enc_flat[...] = back[0].astype(jnp.bfloat16)

    lanes8 = lanes_of((8, LANES))
    per_peer = UNIT // n_dp

    def send_unit(n, left, right):
        for a in range(3):
            for b in range(3):
                acc = jnp.zeros((WIDE, C), jnp.float32)
                for u in range(SPLIT):
                    acc = acc + dot_t(left(u), right(u, a, b))
                t = 3 * a + b
                grads[n, t * WIDE : (t + 1) * WIDE, 0:C] = acc * grad_scale
        for p in range(n_dp):
            block = grads[n, pl.ds(p * per_peer, 8, stride=4), :]
            for g in range(1, 4):
                rows = grads[n, pl.ds(p * per_peer + g, 8, stride=4), :]
                block = jnp.where(lanes8 < 32 * g, block, pltpu.roll(rows, 32 * g, 1))
            terms[n, p] = block.astype(SEND)

        for dx, dz in hops:
            far_copy(n, dx, dz).start()

    columns_of = n_dp // ring

    def steps(d, n):
        return min(d, n - d)

    hops = sorted(
        ((dx, dz) for dx in range(columns_of) for dz in range(ring) if dx or dz),
        key=lambda hop: (-steps(hop[0], columns_of) - steps(hop[1], ring), hop[0] * 3 % 4, hop[1] * 5 % 8),
    )

    def far_copy(n, dx, dz):
        peer = lax.rem(far + dx, columns_of) * ring + lax.rem(near + dz, ring)
        return pltpu.make_async_remote_copy(
            src_ref=terms.at[n, peer], dst_ref=arrived.at[n, me],
            send_sem=far_s.at[n], recv_sem=far_r.at[n], device_id={DP: peer},
        )

    def far_all(n):
        return pltpu.make_async_remote_copy(
            src_ref=terms.at[n, pl.ds(0, n_dp - 1)], dst_ref=arrived.at[n, pl.ds(0, n_dp - 1)],
            send_sem=far_s.at[n], recv_sem=far_r.at[n], device_id={DP: along(1)},
        )

    heard(3)
    halo_arrived(1)
    send_unit(1, lambda u: c3[u], lambda u, a, b: xd[u + b, :, lane(a, FULL)])

    gain = e_gain * e_scale
    skip_arrivals()
    skip_own.wait()
    for j in range(n_space):
        shift = gain * (unpack(stat_got[0, j], 16)[0] * (1.0 / cells) - e_mean) + e_bias
        for w in range(SPLIT):
            at = lane(1 + SPLIT * j + w)
            for u in range(4):
                act = jnp.maximum(gain * xs[u, :, at].astype(jnp.float32) + shift, 0.0)
                if u == 0:
                    act = jnp.where(slab > 0, act, 0.0)
                if u == 3:
                    act = jnp.where(slab < last, act, 0.0)
                xs[u, :, at] = act.astype(jnp.bfloat16)

    send_unit(2, lambda u: c3[u], lambda u, a, b: xs[u + b, :, lane(a, FULL)])

    def hand(k):
        src, dst, step = (
            (enc_flat, enc_out, 1),
            (dec_raw.at[0], dec_got.at[0], -1),
            (dec_raw.at[1], dec_got.at[1], -1),
            (coef_send, coef_got, -1),
        )[k]
        return pltpu.make_async_remote_copy(
            src_ref=src, dst_ref=dst, send_sem=hand_s.at[k], recv_sem=hand_r.at[k],
            device_id={SECTION: level + step},
        )

    first, second = zero, zero
    for u in range(SPLIT):
        for q in range(0, FULL, chunk):
            acc = jnp.zeros((WIDE, chunk * LANES), jnp.float32)
            for b in range(3):
                three = []
                for a in range(3):
                    at = lane(q + a, chunk)
                    three += [xd[u + b, :, at], xs[u + b, :, at]]
                acc = acc + dot(wide_d[b], jnp.concatenate(three, axis=0))
            for r in range(chunk):
                row = merge_taps(acc[:, lane(r)])
                dec_pre[u, :, lane(q + r)] = row
                first = first + row
                second = second + row * row
        if u == 0:
            centre = jnp.sum(first, axis=1, keepdims=True) * (SPLIT / cells)
        else:
            send_stats(2, first, second)
        for v in range(FULL):
            dec_raw[u, :, lane(v)] = (dec_pre[u, :, lane(v)] - centre).astype(jnp.bfloat16)

        @pl.when(level > 0)
        def _():
            hand(1 + u).start()


    @pl.when(level < n_section - 1)
    def _():
        hand(0).start()

    g_mean, gh_mean = all_stats(1)
    for u in range(SPLIT):
        for v in range(FULL):
            hat = enc_hat_of(v, u)
            row = (gated_of(v, u, hat) - g_mean - hat * gh_mean) * e_scale
            row = row.astype(jnp.bfloat16).astype(jnp.float32)
            e3[u, :, lane(v)] = gather_taps(row)
    send_unit(0, lambda u: e3[u], lambda u, a, b: x[u + a, :, lane(b, FULL)])
    d_mean, d_square = all_stats(2)
    d_gain = d_gain * lax.rsqrt(d_square - d_mean * d_mean + EPS)
    coef_send[...] = pack_pair(d_gain, d_gain * (centre - d_mean) + d_bias)

    @pl.when(level > 0)
    def _():
        hand(3).start()

    @pl.when(level == 0)
    def _():
        enc_out[...] = jnp.zeros(enc_out.shape, enc_out.dtype)

    def near_copy(n, i):
        units = pl.ds(1, 2) if n else pl.ds(0, 1)
        k = i - 1 + (n_space - 1) * min(n, 1)
        return pltpu.make_async_remote_copy(
            src_ref=near_send.at[units], dst_ref=near_got.at[i - 1, units],
            send_sem=near_s.at[k], recv_sem=near_r.at[k],
            device_id={SPACE: lax.rem(slab + i, n_space)},
        )

    for n in (1, 2, 0):
        far_all(n).wait_recv()
        arrived[n, me] = terms[n, me]
        sums = [arrived[n, p].astype(jnp.float32) for p in range(n_dp)]
        while len(sums) > 1:
            sums = [a + b for a, b in zip(sums[::2], sums[1::2])]
        near_send[n] = sums[0]
        if n != 1:
            for i in range(1, n_space):
                near_copy(n, i).start()

    @pl.when(level < n_section - 1)
    def _():
        hand(1).wait_recv()
        hand(2).wait_recv()
        hand(3).wait_recv()
        scale, shift = unpack(coef_got[...], 1)
        for u in range(SPLIT):
            for v in range(FULL):
                back[1, pl.ds(v * SPLIT + u, C, stride=ROWS), :] = jnp.maximum(
                    scale * dec_got[u, :, lane(v)].astype(jnp.float32) + shift, 0.0
                )
        dec_out[...] = back[1].astype(jnp.bfloat16)

    @pl.when(level == n_section - 1)
    def _():
        dec_out[...] = jnp.zeros(dec_out.shape, dec_out.dtype)

    acc = near_send[...]
    for i in range(1, n_space):
        for n in (2, 0):
            near_copy(n, i).wait_recv()
        acc = acc + near_got[i - 1]
    total[...] = acc

    @pl.when(level > 0)
    def _():
        hand(0).wait_recv()
        hand(1).wait_send()
        hand(2).wait_send()
        hand(3).wait_send()

    @pl.when(level < n_section - 1)
    def _():
        hand(0).wait_send()

    @pl.when(slab < last)
    def _():
        for k in range(2):
            halo(k, True).wait_send()

    @pl.when(slab > 0)
    def _():
        for k in range(2):
            halo(k, False).wait_send()

    for i in range(1, n_space):
        for n in range(3):
            stat_copy(n, i).wait_send()
        for n in (2, 0):
            near_copy(n, i).wait_send()
    cot_copies(lambda copy: copy.wait_send())
    skip_copies(lambda copy: copy.wait_send())
    for n in range(3):
        far_all(n).wait_send()


def finish(n_space, enc_in, dec_in, sums, enc_hbm, dec_hbm, enc_grad, dec_grad, sems):
    slab = lax.axis_index(SPACE)
    copies = [
        pltpu.make_async_copy(enc_in, enc_hbm, sems.at[0]),
        pltpu.make_async_copy(dec_in, dec_hbm, sems.at[1]),
    ]
    for copy in copies:
        copy.start()

    def part(rows, out):
        flat = jnp.concatenate(rows, axis=1)
        width = out.shape[1]
        mine = flat[:, 0:width]
        for j in range(1, n_space):
            mine = jnp.where(slab == j, flat[:, j * width : (j + 1) * width], mine)
        out[...] = mine

    part([sums[0, r : r + 1, :] for r in range(7)], enc_grad)
    own, skip = sums[1], sums[2]
    group = lanes_of((8, LANES)) // C
    even = jnp.where(
        group == 0, own,
        jnp.where(
            group == 1, pltpu.roll(skip, 32, 1),
            jnp.where(group == 2, pltpu.roll(own, 32, 1), pltpu.roll(skip, 64, 1)),
        ),
    )
    odd = jnp.where(
        group == 0, pltpu.roll(own, 64, 1),
        jnp.where(
            group == 1, pltpu.roll(skip, 96, 1),
            jnp.where(group == 2, pltpu.roll(own, 96, 1), skip),
        ),
    )
    rows = []
    for r in range(7):
        rows += [even[r : r + 1, :], odd[r : r + 1, :]]
    part(rows, dec_grad)
    for copy in copies:
        copy.wait()


def body(
    enc_input, dec_input, dec_cotangent, deep_cotangent,
    enc_weight, dec_weight, enc_gain, enc_bias, dec_gain, dec_bias,
):
    n_section, n_dp, n_space = (lax.axis_size(a) for a in (SECTION, DP, SPACE))
    voxels = enc_input.shape[3] * n_space * enc_input.shape[4] * enc_input.shape[5]
    grad_scale = 1.0 / math.sqrt(n_dp * voxels)
    flat = (C * ROWS, LANES)
    vmem = pl.BlockSpec(memory_space=pltpu.VMEM)
    hbm = pl.BlockSpec(memory_space=pltpu.HBM)
    bf16, f32 = jnp.bfloat16, jnp.float32
    dma = pltpu.SemaphoreType.DMA
    others = n_space - 1
    enc_out, dec_out, total = pl.pallas_call(
        lambda *refs: kernel(n_section, n_dp, n_space, voxels, grad_scale, *refs),
        out_shape=(
            pltpu.VMEM(flat, bf16),
            pltpu.VMEM(flat, bf16),
            pltpu.VMEM((3, 8, LANES), f32),
        ),
        in_specs=[hbm] * 10,
        out_specs=(vmem, vmem, vmem),
        scratch_shapes=[
            pltpu.VMEM((4, *flat), bf16),
            pltpu.VMEM((TAPS, WIDE, C), bf16),
            pltpu.VMEM((TAPS, WIDE, 2 * C), bf16),
            pltpu.VMEM((4, 1, C), f32),
            pltpu.VMEM((4, *flat), f32),
            pltpu.VMEM((2, *flat), f32),
            pltpu.VMEM((4, C, PADDED), bf16),
            pltpu.VMEM((4, C, PADDED), bf16),
            pltpu.VMEM((4, C, PADDED), bf16),
            pltpu.VMEM((4, C, PADDED), bf16),
            pltpu.VMEM((FULL + 2, C, PAIR), bf16),
            pltpu.VMEM((SPLIT, WIDE, RUN), bf16),
            pltpu.VMEM((4, WIDE, PADDED), bf16),
            pltpu.VMEM((SPLIT, WIDE, RUN), bf16),
            pltpu.VMEM((FULL + 2, C, PAIR), bf16),
            pltpu.VMEM((FULL, C, PAIR), bf16),
            pltpu.VMEM((FULL, C, PAIR), f32),
            pltpu.VMEM((FULL, C, PAIR), f32),
            pltpu.VMEM((SPLIT, C, RUN), f32),
            pltpu.VMEM((LANES, LANES), f32),
            pltpu.VMEM((TAPS, C, WIDE), bf16),
            pltpu.VMEM((3, WIDE, 3 * C), bf16),
            pltpu.VMEM((3, WIDE, 6 * C), bf16),
            pltpu.VMEM((3, 8, LANES), f32),
            pltpu.VMEM((3, n_space, 8, LANES), f32),
            pltpu.VMEM((3, UNIT + 8, LANES), f32),
            pltpu.VMEM((3, n_dp, 8, LANES), SEND),
            pltpu.VMEM((3, n_dp, 8, LANES), SEND),
            pltpu.VMEM((3, 8, LANES), f32),
            pltpu.VMEM((others, 3, 8, LANES), f32),
            pltpu.VMEM(flat, bf16),
            pltpu.VMEM((SPLIT, C, RUN), bf16),
            pltpu.VMEM((SPLIT, C, RUN), bf16),
            pltpu.VMEM((8, LANES), f32),
            pltpu.VMEM((8, LANES), f32),
            dma((10,)),
            dma((4,)), dma((4,)),
            dma((3 * others,)), dma((3 * others,)),
            dma((others,)), dma((others,)),
            dma((others,)), dma((others,)),
            dma((2,)),
            dma((4,)), dma((4,)),
            dma((3,)), dma((3,)),
            dma((2 * others,)), dma((2 * others,)),
            pltpu.SemaphoreType.REGULAR((4,)),
        ],
        compiler_params=pltpu.CompilerParams(
            collective_id=0, has_side_effects=True, vmem_limit_bytes=48 * 1024 * 1024
        ),
    )(
        *(
            pltpu.with_memory_space_constraint(array, pltpu.HBM)
            for array in (
                enc_input.reshape(flat), dec_input.reshape(flat), dec_cotangent.reshape(flat),
                deep_cotangent.reshape(flat), enc_weight.reshape(TAPS, WIDE, C),
                dec_weight.reshape(TAPS, WIDE, 2 * C), enc_gain, enc_bias, dec_gain, dec_bias,
            )
        )
    )
    enc_width, dec_width = UNIT * C // (n_dp * n_space), 2 * UNIT * C // (n_dp * n_space)
    enc_out, dec_out, enc_grad, dec_grad = pl.pallas_call(
        lambda *refs: finish(n_space, *refs),
        out_shape=(
            jax.ShapeDtypeStruct(flat, bf16),
            jax.ShapeDtypeStruct(flat, bf16),
            jax.ShapeDtypeStruct((1, enc_width), f32),
            jax.ShapeDtypeStruct((1, dec_width), f32),
        ),
        in_specs=[vmem] * 3,
        out_specs=(hbm, hbm, vmem, vmem),
        scratch_shapes=[dma((2,))],
        compiler_params=pltpu.CompilerParams(vmem_limit_bytes=4 * 1024 * 1024),
    )(enc_out, dec_out, total)
    return (
        enc_out.reshape(enc_input.shape), dec_out.reshape(dec_input.shape), enc_grad, dec_grad
    )


def solution(mesh):
    by_depth = P(SECTION, DP, None, SPACE, None, None)
    by_height = P(SECTION, DP, None, None, SPACE, None)
    whole3, whole1 = P(SECTION, None, None, None), P(SECTION, None)
    return jax.shard_map(
        body,
        mesh=mesh,
        in_specs=(by_depth, by_height, by_height, by_depth, whole3, whole3, *[whole1] * 4),
        out_specs=(by_depth, by_height, P(SECTION, (DP, SPACE)), P(SECTION, (DP, SPACE))),
        check_vma=False,
    )
```

```python
import math

import jax
import jax.numpy as jnp
from jax import lax
from jax.experimental import pallas as pl
from jax.experimental.pallas import tpu as pltpu
from jax.sharding import PartitionSpec as P

SPACE = "space"
DP = "dp"
SECTION = "section"

EPS = 1e-05

C = 32
LANES = 128
FULL = 8
SPLIT = 2
ROWS = FULL * SPLIT
RUN = FULL * LANES
PADDED = (FULL + 2) * LANES
PAIR = SPLIT * LANES
TAPS = 9
WIDE = 3 * C
UNIT = TAPS * WIDE
RING = 8
SEND = jnp.bfloat16


def dot(a, b):
    return jnp.dot(a, b, preferred_element_type=jnp.float32)


def dot_t(a, b):
    return lax.dot_general(a, b, (((1,), (1,)), ((), ())), preferred_element_type=jnp.float32)


def lanes_of(shape):
    return lax.broadcasted_iota(jnp.int32, shape, len(shape) - 1)


def to_right(row):
    return jnp.where(lanes_of(row.shape) == 0, 0.0, pltpu.roll(row, 1, 1))


def to_left(row):
    return jnp.where(lanes_of(row.shape) == LANES - 1, 0.0, pltpu.roll(row, LANES - 1, 1))


def gather_taps(row):
    return jnp.concatenate([to_left(row), row, to_right(row)], axis=0).astype(jnp.bfloat16)


def merge_taps(wide):
    return to_right(wide[0:C]) + wide[C : 2 * C] + to_left(wide[2 * C : 3 * C])


def pack_stats(first, second):
    lanes = lanes_of((8, LANES))
    packed = jnp.zeros((8, LANES), jnp.float32)
    for k in range(4):
        for n, whole in enumerate((first, second)):
            part = whole[8 * k : 8 * k + 8]
            for shift in (64, 32, 16):
                part = part + pltpu.roll(part, shift, 1)
            low = 32 * k + 16 * n
            packed = jnp.where((lanes >= low) & (lanes < low + 16), part, packed)
    return packed


def pack_pair(first, second):
    lanes = lanes_of((8, LANES))
    packed = jnp.zeros((8, LANES), jnp.float32)
    for k in range(4):
        for n, whole in enumerate((first, second)):
            low = 32 * k + 16 * n
            mine = (lanes >= low) & (lanes < low + 16)
            packed = jnp.where(mine, whole[8 * k : 8 * k + 8], packed)
    return packed


def unpack(packed, width):
    lanes = lanes_of((8, LANES))
    both = []
    for n in range(2):
        pieces = []
        for k in range(4):
            low = 32 * k + 16 * n
            mine = jnp.where((lanes >= low) & (lanes < low + width), packed, 0.0)
            pieces.append(jnp.sum(mine, axis=1, keepdims=True))
        both.append(jnp.concatenate(pieces, axis=0))
    return both


def kernel(
    n_section, n_dp, n_space, voxels, grad_scale,
    enc_hbm, dec_hbm, cot_hbm, deep_hbm, enc_w_hbm, dec_w_hbm, g0, g1, g2, g3,
    enc_out, dec_out, total,
    loaded, enc_w, dec_w, params,
    stage, back, x, xd, xs, xc, cot_send, c3, c3e, e3, skip_send, sg, deep, pre, dec_pre,
    prm, tr_w, wide_e, wide_d, stat_send, stat_got, grads, terms, arrived, near_send, near_got,
    enc_flat, dec_raw, dec_got, coef_send, coef_got,
    load_s, halo_s, halo_r, stat_s, stat_r, skip_s, skip_r, cot_s, cot_r, own_sem,
    hand_s, hand_r, far_s, far_r, near_s, near_r, known,
):
    me = lax.axis_index(DP)
    slab = lax.axis_index(SPACE)
    level = lax.axis_index(SECTION)
    last = n_space - 1
    cells = ROWS * LANES

    loads = [
        pltpu.make_async_copy(src, dst, load_s.at[n])
        for n, (src, dst) in enumerate(
            (
                (enc_hbm, loaded.at[0]), (cot_hbm, loaded.at[1]), (enc_w_hbm, enc_w),
                (dec_hbm, loaded.at[2]), (deep_hbm, loaded.at[3]), (dec_w_hbm, dec_w),
                (g0, params.at[0]), (g1, params.at[1]), (g2, params.at[2]), (g3, params.at[3]),
            )
        )
    ]
    for load in loads:
        load.start()

    barrier = pltpu.get_barrier_semaphore()

    ring = min(RING, n_dp)
    far, near = lax.div(me, ring), lax.rem(me, ring)

    def along(step):
        return far * ring + lax.rem(near + step + ring, ring)

    def across(step):
        return lax.rem(far + step + n_dp // ring, n_dp // ring) * ring + near

    def tell(sem, peers):
        for peer in peers:
            pl.semaphore_signal(sem, inc=1, device_id={DP: peer})

    def heard(n):
        pl.semaphore_wait(known.at[n], 2)

    for i in range(1, n_space):
        pl.semaphore_signal(barrier, inc=1, device_id={SPACE: lax.rem(slab + i, n_space)})
    tell(barrier, (along(1), along(-1), across(1), across(-1)))

    @pl.when(level > 0)
    def _():
        pl.semaphore_signal(barrier, inc=1, device_id={SECTION: level - 1})

    @pl.when(level < n_section - 1)
    def _():
        pl.semaphore_signal(barrier, inc=1, device_id={SECTION: level + 1})

    def row_of(k, r):
        return stage[k, pl.ds(r, C, stride=ROWS), :]

    def lane(r, n=1):
        return slice(r * LANES, (r + n) * LANES)

    inner = lane(1, FULL)

    for ref in (x, xd, xs, xc):
        ref[:, :, lane(0)] = jnp.zeros((4, C, LANES), ref.dtype)
        ref[:, :, lane(FULL + 1)] = jnp.zeros((4, C, LANES), ref.dtype)
    c3e[:, :, lane(0)] = jnp.zeros((4, WIDE, LANES), c3e.dtype)
    c3e[:, :, lane(FULL + 1)] = jnp.zeros((4, WIDE, LANES), c3e.dtype)
    for ref in (skip_send, cot_send):
        ref[0] = jnp.zeros((C, PAIR), ref.dtype)
        ref[FULL + 1] = jnp.zeros((C, PAIR), ref.dtype)

    @pl.when(slab == 0)
    def _():
        x[0] = jnp.zeros((C, PADDED), x.dtype)
        xd[0] = jnp.zeros((C, PADDED), xd.dtype)
        xc[0] = jnp.zeros((C, PADDED), xc.dtype)
        xs[0] = jnp.zeros((C, PADDED), xs.dtype)

    @pl.when(slab == last)
    def _():
        x[3] = jnp.zeros((C, PADDED), x.dtype)
        xd[3] = jnp.zeros((C, PADDED), xd.dtype)
        xc[3] = jnp.zeros((C, PADDED), xc.dtype)
        xs[3] = jnp.zeros((C, PADDED), xs.dtype)

    loads[0].wait()
    stage[0] = loaded[0].astype(jnp.float32)
    for u in range(SPLIT):
        for v in range(FULL):
            x[1 + u, :, lane(1 + v)] = row_of(0, u * FULL + v).astype(jnp.bfloat16)
    def halo(k, up):
        src_u, dst_u, peer = (2, 0, slab + 1) if up else (1, 3, slab - 1)
        ref = (x, xd)[k]
        n = 2 * k + (0 if up else 1)
        return pltpu.make_async_remote_copy(
            src_ref=ref.at[src_u, :, inner], dst_ref=ref.at[dst_u, :, inner],
            send_sem=halo_s.at[n], recv_sem=halo_r.at[n], device_id={SPACE: peer},
        )

    def halo_start(k):
        @pl.when(slab < last)
        def _():
            halo(k, True).start()

        @pl.when(slab > 0)
        def _():
            halo(k, False).start()

    def halo_arrived(k):
        @pl.when(slab > 0)
        def _():
            halo(k, True).wait_recv()

        @pl.when(slab < last)
        def _():
            halo(k, False).wait_recv()

    def regroup(sender, receiver, send_sem, recv_sem, own):
        def refs(source, target, first, count):
            at = pl.multiple_of((1 + source * SPLIT) * LANES, LANES)
            return (
                sender.at[pl.ds(target * SPLIT + first, count)],
                receiver.at[pl.ds(first, count), :, pl.ds(at, PAIR)],
            )

        def remote(i, peer, source, target, first, count):
            src, dst = refs(source, target, first, count)
            return pltpu.make_async_remote_copy(
                src_ref=src, dst_ref=dst, send_sem=send_sem.at[i - 1],
                recv_sem=recv_sem.at[i - 1], device_id={SPACE: peer},
            )

        def copies(act):
            for i in range(1, n_space):
                peer = lax.rem(slab + i, n_space)
                by_end(peer, lambda *cut: act(remote(i, peer, slab, peer, *cut)))

        def arrivals():
            for i in range(1, n_space):
                peer = lax.rem(slab - i + n_space, n_space)
                by_end(slab, lambda *cut: remote(i, peer, peer, slab, *cut).wait_recv())

        return copies, arrivals, pltpu.make_async_copy(*refs(slab, slab, 0, SPLIT + 2), own)

    def by_end(target, act):
        @pl.when(target == 0)
        def _():
            act(1, SPLIT + 1)

        @pl.when(target == last)
        def _():
            act(0, SPLIT + 1)

        @pl.when((target > 0) & (target < last))
        def _():
            act(0, SPLIT + 2)

    cot_copies, cot_arrivals, cot_own = regroup(cot_send, xc, cot_s, cot_r, own_sem.at[0])
    skip_copies, skip_arrivals, skip_own = regroup(skip_send, xs, skip_s, skip_r, own_sem.at[1])

    pl.semaphore_wait(
        barrier, 4 + n_space - 1 + lax.min(level, 1) + lax.min(n_section - 1 - level, 1)
    )
    halo_start(0)
    tell(known.at[0], (along(1), along(-1)))
    loads[1].wait()
    stage[1] = loaded[1].astype(jnp.float32)
    for u in range(SPLIT):
        for v in range(FULL):
            cot_send[1 + v, :, lane(u)] = row_of(1, v * SPLIT + u).astype(jnp.bfloat16)
    cot_copies(lambda copy: copy.start())
    cot_own.start()
    loads[3].wait()
    stage[2] = loaded[2].astype(jnp.float32)
    for u in range(SPLIT):
        for v in range(FULL):
            xd[1 + u, :, lane(1 + v)] = row_of(2, v * SPLIT + u).astype(jnp.bfloat16)

    halo_start(1)

    for n in (6, 7, 8, 9):
        loads[n].wait()
    prm[...] = jnp.zeros((LANES, LANES), jnp.float32)
    for n in range(4):
        prm[n : n + 1, 0:C] = params[n]
    columns = prm[...].T
    e_gain, e_bias = columns[0:C, 0:1], columns[0:C, 1:2]
    d_gain, d_bias = columns[0:C, 2:3], columns[0:C, 3:4]
    pick = (
        lax.broadcasted_iota(jnp.int32, (C, 2 * C), 1)
        == lax.broadcasted_iota(jnp.int32, (C, 2 * C), 0) + C
    ).astype(jnp.bfloat16)
    loads[5].wait()
    for t in range(TAPS):
        tr_w[t] = dot_t(pick, dec_w[t]).astype(jnp.bfloat16)
    loads[2].wait()
    for k in range(3):
        wide_e[k] = jnp.concatenate([enc_w[3 * k + b] for b in range(3)], axis=1)
        wide_d[k] = jnp.concatenate([dec_w[3 * a + k] for a in range(3)], axis=1)
    loads[4].wait()
    stage[3] = loaded[3].astype(jnp.float32)
    for u in range(SPLIT):
        for v in range(FULL):
            c3[u, :, lane(v)] = gather_taps(row_of(1, v * SPLIT + u))
            deep[v, :, lane(u)] = row_of(3, u * FULL + v)
    heard(0)
    tell(known.at[1], (along(2), along(-2)))

    zero = jnp.zeros((C, LANES), jnp.float32)
    chunk = 4

    halo_arrived(0)
    first, second = zero, zero
    for u in range(SPLIT):
        for q in range(0, FULL, chunk):
            acc = jnp.zeros((WIDE, chunk * LANES), jnp.float32)
            for a in range(3):
                three = [x[u + a, :, lane(q + b, chunk)] for b in range(3)]
                acc = acc + dot(wide_e[a], jnp.concatenate(three, axis=0))
            for r in range(chunk):
                row = merge_taps(acc[:, lane(r)])
                pre[q + r, :, lane(u)] = row
                first = first + row
                second = second + row * row

    def stat_copy(n, i):
        k = n * (n_space - 1) + i - 1
        return pltpu.make_async_remote_copy(
            src_ref=stat_send.at[n], dst_ref=stat_got.at[n, slab],
            send_sem=stat_s.at[k], recv_sem=stat_r.at[k],
            device_id={SPACE: lax.rem(slab + i, n_space)},
        )

    def stat_arrival(n, i):
        k = n * (n_space - 1) + i - 1
        peer = lax.rem(slab - i + n_space, n_space)
        return pltpu.make_async_remote_copy(
            src_ref=stat_send.at[n], dst_ref=stat_got.at[n, peer],
            send_sem=stat_s.at[k], recv_sem=stat_r.at[k], device_id={SPACE: peer},
        )

    def send_stats(n, first, second):
        packed = pack_stats(first, second)
        stat_send[n] = packed
        for i in range(1, n_space):
            stat_copy(n, i).start()
        stat_got[n, slab] = packed
        return packed

    def all_stats(n):
        for i in range(1, n_space):
            stat_arrival(n, i).wait_recv()
        packed = stat_got[n, 0]
        for j in range(1, n_space):
            packed = packed + stat_got[n, j]
        one, two = unpack(packed, 16)
        return one * (1.0 / voxels), two * (1.0 / voxels)

    packed = send_stats(0, first, second)
    own_mean = unpack(packed, 16)[0] * (1.0 / cells)
    for v in range(FULL):
        for u in range(SPLIT):
            skip_send[1 + v, :, lane(u)] = (pre[v, :, lane(u)] - own_mean).astype(jnp.bfloat16)
    skip_copies(lambda copy: copy.start())
    skip_own.start()
    heard(1)
    tell(known.at[2], (across(1), across(-1)))

    cot_arrivals()
    cot_own.wait()
    for u in range(4):
        for v in range(FULL):
            c3e[u, :, lane(1 + v)] = gather_taps(xc[u, :, lane(1 + v)].astype(jnp.float32))
    for u in range(SPLIT):
        for q in range(0, FULL, chunk):
            acc = jnp.zeros((C, chunk * LANES), jnp.float32)
            for a in range(3):
                for b in range(3):
                    acc = acc + dot(tr_w[3 * a + b], c3e[u + 2 - a, :, lane(q + 2 - b, chunk)])
            for r in range(chunk):
                sg[q + r, :, lane(u)] = acc[:, lane(r)].astype(jnp.bfloat16)

    heard(2)
    tell(known.at[3], (across(1), across(-1)))

    e_mean, e_square = all_stats(0)
    e_scale = lax.rsqrt(e_square - e_mean * e_mean + EPS)

    def enc_hat_of(v, u):
        return (pre[v, :, lane(u)] - e_mean) * e_scale

    def gated_of(v, u, hat):
        upstream = sg[v, :, lane(u)].astype(jnp.float32) + deep[v, :, lane(u)]
        return jnp.where(e_gain * hat + e_bias > 0, upstream, 0.0) * e_gain

    first, second = zero, zero
    for v in range(FULL):
        for u in range(SPLIT):
            hat = enc_hat_of(v, u)
            gated = gated_of(v, u, hat)
            first = first + gated
            second = second + gated * hat
    send_stats(1, first, second)
    for v in range(FULL):
        for u in range(SPLIT):
            back[0, pl.ds(u * FULL + v, C, stride=ROWS), :] = jnp.maximum(
                e_gain * enc_hat_of(v, u) + e_bias, 0.0
            )
    enc_flat[...] = back[0].astype(jnp.bfloat16)

    lanes8 = lanes_of((8, LANES))
    per_peer = UNIT // n_dp

    def send_unit(n, left, right):
        for a in range(3):
            for b in range(3):
                acc = jnp.zeros((WIDE, C), jnp.float32)
                for u in range(SPLIT):
                    acc = acc + dot_t(left(u), right(u, a, b))
                t = 3 * a + b
                grads[n, t * WIDE : (t + 1) * WIDE, 0:C] = acc * grad_scale
        for p in range(n_dp):
            block = grads[n, pl.ds(p * per_peer, 8, stride=4), :]
            for g in range(1, 4):
                rows = grads[n, pl.ds(p * per_peer + g, 8, stride=4), :]
                block = jnp.where(lanes8 < 32 * g, block, pltpu.roll(rows, 32 * g, 1))
            terms[n, p] = block.astype(SEND)

        for dx, dz in hops:
            far_copy(n, dx, dz).start()

    columns_of = n_dp // ring

    def steps(d, n):
        return min(d, n - d)

    hops = sorted(
        ((dx, dz) for dx in range(columns_of) for dz in range(ring) if dx or dz),
        key=lambda hop: (-steps(hop[1], ring), -steps(hop[0], columns_of), hop[1]),
    )

    def far_copy(n, dx, dz):
        peer = lax.rem(far + dx, columns_of) * ring + lax.rem(near + dz, ring)
        return pltpu.make_async_remote_copy(
            src_ref=terms.at[n, peer], dst_ref=arrived.at[n, me],
            send_sem=far_s.at[n], recv_sem=far_r.at[n], device_id={DP: peer},
        )

    def far_all(n):
        return pltpu.make_async_remote_copy(
            src_ref=terms.at[n, pl.ds(0, n_dp - 1)], dst_ref=arrived.at[n, pl.ds(0, n_dp - 1)],
            send_sem=far_s.at[n], recv_sem=far_r.at[n], device_id={DP: along(1)},
        )

    heard(3)
    halo_arrived(1)
    send_unit(1, lambda u: c3[u], lambda u, a, b: xd[u + b, :, lane(a, FULL)])

    gain = e_gain * e_scale
    skip_arrivals()
    skip_own.wait()
    for j in range(n_space):
        shift = gain * (unpack(stat_got[0, j], 16)[0] * (1.0 / cells) - e_mean) + e_bias
        for w in range(SPLIT):
            at = lane(1 + SPLIT * j + w)
            for u in range(4):
                act = jnp.maximum(gain * xs[u, :, at].astype(jnp.float32) + shift, 0.0)
                if u == 0:
                    act = jnp.where(slab > 0, act, 0.0)
                if u == 3:
                    act = jnp.where(slab < last, act, 0.0)
                xs[u, :, at] = act.astype(jnp.bfloat16)

    send_unit(2, lambda u: c3[u], lambda u, a, b: xs[u + b, :, lane(a, FULL)])

    def hand(k):
        src, dst, step = (
            (enc_flat, enc_out, 1),
            (dec_raw.at[0], dec_got.at[0], -1),
            (dec_raw.at[1], dec_got.at[1], -1),
            (coef_send, coef_got, -1),
        )[k]
        return pltpu.make_async_remote_copy(
            src_ref=src, dst_ref=dst, send_sem=hand_s.at[k], recv_sem=hand_r.at[k],
            device_id={SECTION: level + step},
        )

    first, second = zero, zero
    for u in range(SPLIT):
        for q in range(0, FULL, chunk):
            acc = jnp.zeros((WIDE, chunk * LANES), jnp.float32)
            for b in range(3):
                three = []
                for a in range(3):
                    at = lane(q + a, chunk)
                    three += [xd[u + b, :, at], xs[u + b, :, at]]
                acc = acc + dot(wide_d[b], jnp.concatenate(three, axis=0))
            for r in range(chunk):
                row = merge_taps(acc[:, lane(r)])
                dec_pre[u, :, lane(q + r)] = row
                first = first + row
                second = second + row * row
        if u == 0:
            centre = jnp.sum(first, axis=1, keepdims=True) * (SPLIT / cells)
        else:
            send_stats(2, first, second)
        for v in range(FULL):
            dec_raw[u, :, lane(v)] = (dec_pre[u, :, lane(v)] - centre).astype(jnp.bfloat16)

        @pl.when(level > 0)
        def _():
            hand(1 + u).start()


    @pl.when(level < n_section - 1)
    def _():
        hand(0).start()

    g_mean, gh_mean = all_stats(1)
    for u in range(SPLIT):
        for v in range(FULL):
            hat = enc_hat_of(v, u)
            row = (gated_of(v, u, hat) - g_mean - hat * gh_mean) * e_scale
            row = row.astype(jnp.bfloat16).astype(jnp.float32)
            e3[u, :, lane(v)] = gather_taps(row)
    send_unit(0, lambda u: e3[u], lambda u, a, b: x[u + a, :, lane(b, FULL)])
    d_mean, d_square = all_stats(2)
    d_gain = d_gain * lax.rsqrt(d_square - d_mean * d_mean + EPS)
    coef_send[...] = pack_pair(d_gain, d_gain * (centre - d_mean) + d_bias)

    @pl.when(level > 0)
    def _():
        hand(3).start()

    @pl.when(level == 0)
    def _():
        enc_out[...] = jnp.zeros(enc_out.shape, enc_out.dtype)

    def near_copy(n, i):
        units = pl.ds(1, 2) if n else pl.ds(0, 1)
        k = i - 1 + (n_space - 1) * min(n, 1)
        return pltpu.make_async_remote_copy(
            src_ref=near_send.at[units], dst_ref=near_got.at[i - 1, units],
            send_sem=near_s.at[k], recv_sem=near_r.at[k],
            device_id={SPACE: lax.rem(slab + i, n_space)},
        )

    for n in (1, 2, 0):
        far_all(n).wait_recv()
        arrived[n, me] = terms[n, me]
        sums = [arrived[n, p].astype(jnp.float32) for p in range(n_dp)]
        while len(sums) > 1:
            sums = [a + b for a, b in zip(sums[::2], sums[1::2])]
        near_send[n] = sums[0]
        if n != 1:
            for i in range(1, n_space):
                near_copy(n, i).start()

    @pl.when(level < n_section - 1)
    def _():
        hand(1).wait_recv()
        hand(2).wait_recv()
        hand(3).wait_recv()
        scale, shift = unpack(coef_got[...], 1)
        for u in range(SPLIT):
            for v in range(FULL):
                back[1, pl.ds(v * SPLIT + u, C, stride=ROWS), :] = jnp.maximum(
                    scale * dec_got[u, :, lane(v)].astype(jnp.float32) + shift, 0.0
                )
        dec_out[...] = back[1].astype(jnp.bfloat16)

    @pl.when(level == n_section - 1)
    def _():
        dec_out[...] = jnp.zeros(dec_out.shape, dec_out.dtype)

    acc = near_send[...]
    for i in range(1, n_space):
        for n in (2, 0):
            near_copy(n, i).wait_recv()
        acc = acc + near_got[i - 1]
    total[...] = acc

    @pl.when(level > 0)
    def _():
        hand(0).wait_recv()
        hand(1).wait_send()
        hand(2).wait_send()
        hand(3).wait_send()

    @pl.when(level < n_section - 1)
    def _():
        hand(0).wait_send()

    @pl.when(slab < last)
    def _():
        for k in range(2):
            halo(k, True).wait_send()

    @pl.when(slab > 0)
    def _():
        for k in range(2):
            halo(k, False).wait_send()

    for i in range(1, n_space):
        for n in range(3):
            stat_copy(n, i).wait_send()
        for n in (2, 0):
            near_copy(n, i).wait_send()
    cot_copies(lambda copy: copy.wait_send())
    skip_copies(lambda copy: copy.wait_send())
    for n in range(3):
        far_all(n).wait_send()


def finish(n_space, enc_in, dec_in, sums, enc_hbm, dec_hbm, enc_grad, dec_grad, sems):
    slab = lax.axis_index(SPACE)
    copies = [
        pltpu.make_async_copy(enc_in, enc_hbm, sems.at[0]),
        pltpu.make_async_copy(dec_in, dec_hbm, sems.at[1]),
    ]
    for copy in copies:
        copy.start()

    def part(rows, out):
        flat = jnp.concatenate(rows, axis=1)
        width = out.shape[1]
        mine = flat[:, 0:width]
        for j in range(1, n_space):
            mine = jnp.where(slab == j, flat[:, j * width : (j + 1) * width], mine)
        out[...] = mine

    part([sums[0, r : r + 1, :] for r in range(7)], enc_grad)
    own, skip = sums[1], sums[2]
    group = lanes_of((8, LANES)) // C
    even = jnp.where(
        group == 0, own,
        jnp.where(
            group == 1, pltpu.roll(skip, 32, 1),
            jnp.where(group == 2, pltpu.roll(own, 32, 1), pltpu.roll(skip, 64, 1)),
        ),
    )
    odd = jnp.where(
        group == 0, pltpu.roll(own, 64, 1),
        jnp.where(
            group == 1, pltpu.roll(skip, 96, 1),
            jnp.where(group == 2, pltpu.roll(own, 96, 1), skip),
        ),
    )
    rows = []
    for r in range(7):
        rows += [even[r : r + 1, :], odd[r : r + 1, :]]
    part(rows, dec_grad)
    for copy in copies:
        copy.wait()


def body(
    enc_input, dec_input, dec_cotangent, deep_cotangent,
    enc_weight, dec_weight, enc_gain, enc_bias, dec_gain, dec_bias,
):
    n_section, n_dp, n_space = (lax.axis_size(a) for a in (SECTION, DP, SPACE))
    voxels = enc_input.shape[3] * n_space * enc_input.shape[4] * enc_input.shape[5]
    grad_scale = 1.0 / math.sqrt(n_dp * voxels)
    flat = (C * ROWS, LANES)
    vmem = pl.BlockSpec(memory_space=pltpu.VMEM)
    hbm = pl.BlockSpec(memory_space=pltpu.HBM)
    bf16, f32 = jnp.bfloat16, jnp.float32
    dma = pltpu.SemaphoreType.DMA
    others = n_space - 1
    enc_out, dec_out, total = pl.pallas_call(
        lambda *refs: kernel(n_section, n_dp, n_space, voxels, grad_scale, *refs),
        out_shape=(
            pltpu.VMEM(flat, bf16),
            pltpu.VMEM(flat, bf16),
            pltpu.VMEM((3, 8, LANES), f32),
        ),
        in_specs=[hbm] * 10,
        out_specs=(vmem, vmem, vmem),
        scratch_shapes=[
            pltpu.VMEM((4, *flat), bf16),
            pltpu.VMEM((TAPS, WIDE, C), bf16),
            pltpu.VMEM((TAPS, WIDE, 2 * C), bf16),
            pltpu.VMEM((4, 1, C), f32),
            pltpu.VMEM((4, *flat), f32),
            pltpu.VMEM((2, *flat), f32),
            pltpu.VMEM((4, C, PADDED), bf16),
            pltpu.VMEM((4, C, PADDED), bf16),
            pltpu.VMEM((4, C, PADDED), bf16),
            pltpu.VMEM((4, C, PADDED), bf16),
            pltpu.VMEM((FULL + 2, C, PAIR), bf16),
            pltpu.VMEM((SPLIT, WIDE, RUN), bf16),
            pltpu.VMEM((4, WIDE, PADDED), bf16),
            pltpu.VMEM((SPLIT, WIDE, RUN), bf16),
            pltpu.VMEM((FULL + 2, C, PAIR), bf16),
            pltpu.VMEM((FULL, C, PAIR), bf16),
            pltpu.VMEM((FULL, C, PAIR), f32),
            pltpu.VMEM((FULL, C, PAIR), f32),
            pltpu.VMEM((SPLIT, C, RUN), f32),
            pltpu.VMEM((LANES, LANES), f32),
            pltpu.VMEM((TAPS, C, WIDE), bf16),
            pltpu.VMEM((3, WIDE, 3 * C), bf16),
            pltpu.VMEM((3, WIDE, 6 * C), bf16),
            pltpu.VMEM((3, 8, LANES), f32),
            pltpu.VMEM((3, n_space, 8, LANES), f32),
            pltpu.VMEM((3, UNIT + 8, LANES), f32),
            pltpu.VMEM((3, n_dp, 8, LANES), SEND),
            pltpu.VMEM((3, n_dp, 8, LANES), SEND),
            pltpu.VMEM((3, 8, LANES), f32),
            pltpu.VMEM((others, 3, 8, LANES), f32),
            pltpu.VMEM(flat, bf16),
            pltpu.VMEM((SPLIT, C, RUN), bf16),
            pltpu.VMEM((SPLIT, C, RUN), bf16),
            pltpu.VMEM((8, LANES), f32),
            pltpu.VMEM((8, LANES), f32),
            dma((10,)),
            dma((4,)), dma((4,)),
            dma((3 * others,)), dma((3 * others,)),
            dma((others,)), dma((others,)),
            dma((others,)), dma((others,)),
            dma((2,)),
            dma((4,)), dma((4,)),
            dma((3,)), dma((3,)),
            dma((2 * others,)), dma((2 * others,)),
            pltpu.SemaphoreType.REGULAR((4,)),
        ],
        compiler_params=pltpu.CompilerParams(
            collective_id=0, has_side_effects=True, vmem_limit_bytes=48 * 1024 * 1024
        ),
    )(
        *(
            pltpu.with_memory_space_constraint(array, pltpu.HBM)
            for array in (
                enc_input.reshape(flat), dec_input.reshape(flat), dec_cotangent.reshape(flat),
                deep_cotangent.reshape(flat), enc_weight.reshape(TAPS, WIDE, C),
                dec_weight.reshape(TAPS, WIDE, 2 * C), enc_gain, enc_bias, dec_gain, dec_bias,
            )
        )
    )
    enc_width, dec_width = UNIT * C // (n_dp * n_space), 2 * UNIT * C // (n_dp * n_space)
    enc_out, dec_out, enc_grad, dec_grad = pl.pallas_call(
        lambda *refs: finish(n_space, *refs),
        out_shape=(
            jax.ShapeDtypeStruct(flat, bf16),
            jax.ShapeDtypeStruct(flat, bf16),
            jax.ShapeDtypeStruct((1, enc_width), f32),
            jax.ShapeDtypeStruct((1, dec_width), f32),
        ),
        in_specs=[vmem] * 3,
        out_specs=(hbm, hbm, vmem, vmem),
        scratch_shapes=[dma((2,))],
        compiler_params=pltpu.CompilerParams(vmem_limit_bytes=4 * 1024 * 1024),
    )(enc_out, dec_out, total)
    return (
        enc_out.reshape(enc_input.shape), dec_out.reshape(dec_input.shape), enc_grad, dec_grad
    )


def solution(mesh):
    by_depth = P(SECTION, DP, None, SPACE, None, None)
    by_height = P(SECTION, DP, None, None, SPACE, None)
    whole3, whole1 = P(SECTION, None, None, None), P(SECTION, None)
    return jax.shard_map(
        body,
        mesh=mesh,
        in_specs=(by_depth, by_height, by_height, by_depth, whole3, whole3, *[whole1] * 4),
        out_specs=(by_depth, by_height, P(SECTION, (DP, SPACE)), P(SECTION, (DP, SPACE))),
        check_vma=False,
    )
```
